8 devices in a mesh: emb: 8 (over z, y, x, core).
Axes of the slice: x: 2, y: 2, z: 1, core: 2. Of those that a mesh axis runs over, the one named last changes fastest.
Arguments:
- x_start: bfloat16 [16384, 768], P('emb')
- d_out: bfloat16 [16384, 768], P('emb')
- token_ids: int32 [2, 16384, 1], P(None, 'emb')
- w_up: bfloat16 [8, 768, 3072], replicated
- w_down: bfloat16 [8, 3072, 768], replicated
- w_gate: bfloat16 [2, 768, 768], replicated
- w_proj: bfloat16 [2, 768, 768], replicated
- tables: bfloat16 [2, 50304, 768], P(None, 'emb')
Outputs:
- output 1: bfloat16 [16384, 768], P('emb')
- output 2: float32 [2, 50304, 768], P(None, 'emb')
All inputs are finite; a program needn't handle non-finite values.
Results may differ from the reference program's by a relative error of at most 0.02.
Values are sent between devices in bfloat16 or wider.
A program may use at most 1 GiB of HBM per device.

```python
import jax
import jax.numpy as jnp
from jax import lax

D = 768
FF = 3072
HEADS = 1
DH = 768
VH = 50304
LAYERS = 8
TOK = 2048
GROUP = 8
ZIPF_TOP = 16777216
ZIPF_SPAN = 262144
HASH_MUL = 2503

TOKENS = TOK * GROUP
ROWS_DEV = VH // GROUP
CAP = max(8, (4 * TOK * HEADS) // GROUP)
WIDE = HEADS * DH
EPS = 1e-6


def draw_block(key_blk, hot_owner, offset):
    key_perm, key_mix, key_rank = jax.random.split(key_blk, 3)
    spare_slot = jax.random.permutation(key_perm, (GROUP - 1) * CAP)[: TOK * HEADS - CAP]
    spare_owner = spare_slot // CAP
    spare_owner = spare_owner + (spare_owner >= hot_owner).astype(jnp.int32)
    owner_ids = jnp.concatenate([jnp.full((CAP,), hot_owner, jnp.int32), spare_owner.astype(jnp.int32)])
    owner_ids = jax.random.permutation(key_mix, owner_ids)
    uniform_draw = jax.random.randint(key_rank, (TOK * HEADS,), 1, ZIPF_SPAN + 1)
    zipf_rank = ZIPF_TOP // uniform_draw
    local_ids = ((zipf_rank % ROWS_DEV) * HASH_MUL + offset) % ROWS_DEV
    return (owner_ids * ROWS_DEV + local_ids).astype(jnp.int32).reshape(TOK, HEADS)


def draw_table(key_tab, hot_owner, offset):
    dev_keys = jax.random.split(key_tab, GROUP)
    blocks = jax.vmap(draw_block, in_axes=(0, None, None))(dev_keys, hot_owner, offset)
    return blocks.reshape(TOKENS, HEADS)


def draw_ids(key_ids):
    key_hot, key_off, key_tab = jax.random.split(key_ids, 3)
    hot_owner = jax.random.randint(key_hot, (2,), 0, GROUP)
    offset = jax.random.randint(key_off, (2,), 0, ROWS_DEV)
    return jax.vmap(draw_table)(jax.random.split(key_tab, 2), hot_owner, offset).astype(jnp.int32)


def setup_inputs(seed: int = 0) -> dict:
    key_list = jax.random.split(jax.random.key(seed), 8)
    x_start = jax.random.normal(key_list[0], (TOKENS, D), jnp.float32).astype(jnp.bfloat16)
    d_out = jax.random.normal(key_list[1], (TOKENS, D), jnp.float32).astype(jnp.bfloat16)
    token_ids = draw_ids(key_list[2])
    w_up = (jax.random.normal(key_list[3], (LAYERS, D, FF), jnp.float32) * D ** -0.5).astype(jnp.bfloat16)
    w_down = (jax.random.normal(key_list[4], (LAYERS, FF, D), jnp.float32) * (0.5 * FF ** -0.5)).astype(jnp.bfloat16)
    w_gate = (jax.random.normal(key_list[5], (2, D, WIDE), jnp.float32) * D ** -0.5).astype(jnp.bfloat16)
    w_proj = (jax.random.normal(key_list[6], (2, WIDE, D), jnp.float32) * (0.5 * WIDE ** -0.5)).astype(jnp.bfloat16)
    tables = jax.random.normal(key_list[7], (2, VH, DH), jnp.float32).astype(jnp.bfloat16)
    return {'x_start': x_start, 'd_out': d_out, 'token_ids': token_ids, 'w_up': w_up, 'w_down': w_down, 'w_gate': w_gate, 'w_proj': w_proj, 'tables': tables}


def gelu_fn(pre_act):
    return jax.nn.gelu(pre_act, approximate=True)


def gelu_grad(pre_act, cotangent):
    _, pullback = jax.vjp(gelu_fn, pre_act.astype(jnp.float32))
    return pullback(cotangent)[0]


def norm_fwd(x_res):
    x_f = x_res.astype(jnp.float32)
    inv_rms = lax.rsqrt(jnp.mean(x_f * x_f, axis=-1, keepdims=True) + EPS)
    return (x_f * inv_rms).astype(jnp.bfloat16), inv_rms


def norm_bwd(x_res, inv_rms, d_norm):
    x_f = x_res.astype(jnp.float32)
    mean_dot = jnp.mean(x_f * d_norm, axis=-1, keepdims=True)
    return inv_rms * d_norm - x_f * (inv_rms * inv_rms * inv_rms) * mean_dot


def block_pass(block_in, w_up, w_down, w_gate, w_proj, tables):
    x_blk, dy_blk, ids_blk = block_in
    slot_of = {1: 0, LAYERS - 1: 1}
    emb_rows = [tables[which][ids_blk[which]].reshape(TOK, WIDE) for which in range(2)]
    saved_acts = []
    x_cur = x_blk
    for layer_idx in range(LAYERS):
        normed, inv_rms = norm_fwd(x_cur)
        hidden = jnp.dot(normed, w_up[layer_idx], preferred_element_type=jnp.float32).astype(jnp.bfloat16)
        activated = gelu_fn(hidden.astype(jnp.float32)).astype(jnp.bfloat16)
        mlp_out = jnp.dot(activated, w_down[layer_idx], preferred_element_type=jnp.float32).astype(jnp.bfloat16)
        new_res = x_cur.astype(jnp.float32) + mlp_out.astype(jnp.float32)
        gate_saved = None
        if layer_idx in slot_of:
            which = slot_of[layer_idx]
            pre_gate = jnp.dot(normed, w_gate[which], preferred_element_type=jnp.float32).astype(jnp.bfloat16)
            gate_val = gelu_fn(pre_gate.astype(jnp.float32)).astype(jnp.bfloat16)
            mixed_val = (gate_val.astype(jnp.float32) * emb_rows[which].astype(jnp.float32)).astype(jnp.bfloat16)
            proj_out = jnp.dot(mixed_val, w_proj[which], preferred_element_type=jnp.float32).astype(jnp.bfloat16)
            new_res = new_res + proj_out.astype(jnp.float32)
            gate_saved = (pre_gate, gate_val)
        saved_acts.append((x_cur, inv_rms, hidden, gate_saved))
        x_cur = new_res.astype(jnp.bfloat16)
    d_res = dy_blk.astype(jnp.float32)
    pieces = [None, None]
    for layer_idx in reversed(range(1, LAYERS)):
        x_prev, inv_rms, hidden, gate_saved = saved_acts[layer_idx]
        d_low = d_res.astype(jnp.bfloat16)
        if gate_saved is not None:
            which = slot_of[layer_idx]
            pre_gate, gate_val = gate_saved
            d_mix = jnp.dot(d_low, w_proj[which].T, preferred_element_type=jnp.float32)
            pieces[which] = (gate_val.astype(jnp.float32) * d_mix).reshape(TOK, HEADS, DH)
        if layer_idx > 1:
            d_act = jnp.dot(d_low, w_down[layer_idx].T, preferred_element_type=jnp.float32)
            d_hid = gelu_grad(hidden, d_act)
            d_norm = jnp.dot(d_hid.astype(jnp.bfloat16), w_up[layer_idx].T, preferred_element_type=jnp.float32)
            if gate_saved is not None:
                d_gate = gelu_grad(pre_gate, d_mix * emb_rows[which].astype(jnp.float32))
                d_norm = d_norm + jnp.dot(d_gate.astype(jnp.bfloat16), w_gate[which].T, preferred_element_type=jnp.float32)
            d_res = d_res + norm_bwd(x_prev, inv_rms, d_norm)
    return x_cur, jnp.stack(pieces)


def reference(x_start, d_out, token_ids, w_up, w_down, w_gate, w_proj, tables):
    def run_block(block_in):
        return block_pass(block_in, w_up, w_down, w_gate, w_proj, tables)
    ids_blocks = jnp.transpose(token_ids.reshape(2, GROUP, TOK, HEADS), (1, 0, 2, 3))
    x_blocks, grad_rows = lax.map(run_block, (x_start.reshape(GROUP, TOK, D), d_out.reshape(GROUP, TOK, D), ids_blocks))
    d_tables = jnp.stack([jax.ops.segment_sum(grad_rows[:, which].reshape(TOKENS * HEADS, DH), token_ids[which].reshape(TOKENS * HEADS), num_segments=VH) for which in range(2)])
    return x_blocks.reshape(TOKENS, D), d_tables
```

```python
import functools

import jax
import jax.numpy as jnp
from jax import lax
from jax.experimental import pallas as pl
from jax.experimental.pallas import tpu as pltpu
from jax.sharding import PartitionSpec as P

EPS = 1e-6
GELU_K = 0.7978845608028654
GELU_C = 0.044715
F32 = jnp.float32
BF16 = jnp.bfloat16
UNIT = 16
LANE = 128
MAIN = 128
OVER = 384
NT = (((1,), (1,)), ((), ()))
NN = (((1,), (0,)), ((), ()))


def dot(a, b, dims=NN):
    return lax.dot_general(a, b, dims, preferred_element_type=F32)


def gelu(v):
    return v * (0.5 * (1.0 + jnp.tanh(GELU_K * (v + GELU_C * (v * v * v)))))


def gelu_grad(v):
    sq = v * v
    th = jnp.tanh(GELU_K * v * (1.0 + GELU_C * sq))
    return 0.5 * (1.0 + th) + (0.5 * v) * (1.0 - th * th) * (GELU_K + (3.0 * GELU_K * GELU_C) * sq)


def params(mb, sem=None):
    return pltpu.CompilerParams(vmem_limit_bytes=mb * 1024 * 1024, dimension_semantics=sem)


def cost(flops, nbytes):
    return pl.CostEstimate(flops=int(flops), bytes_accessed=int(nbytes), transcendentals=0)


def fwd_body(n_lay, tile, chunk, save_h, x0_ref, up_ref, dn_ref, gate_ref, *rest):
    if save_h:
        x_out, h_out, m_out, a_out, x_sc = rest
    else:
        x_out, m_out, a_out, x_sc = rest
    lay, blk = pl.program_id(0), pl.program_id(1)
    rows = pl.ds(pl.multiple_of(blk * tile, tile), tile)

    @pl.when(lay == 0)
    def _():
        x_sc[rows, :] = x0_ref[...]

    x_bf = x_sc[rows, :]
    x_out[0] = x_bf
    x_f = x_bf.astype(F32)
    inv = lax.rsqrt(jnp.mean(x_f * x_f, axis=-1, keepdims=True) + EPS)
    u = (x_f * inv).astype(BF16)
    acc = None
    for lo in range(0, up_ref.shape[2], chunk):
        h = dot(u, up_ref[0, :, lo:lo + chunk]).astype(BF16)
        if save_h:
            h_out[0, :, lo:lo + chunk] = h
        act = gelu(h.astype(F32)).astype(BF16)
        part = dot(act, dn_ref[0, lo:lo + chunk, :])
        acc = part if acc is None else acc + part
    m = acc.astype(BF16)

    @pl.when(lay < n_lay - 1)
    def _():
        x_sc[rows, :] = (x_f + m.astype(F32)).astype(BF16)

    @pl.when(lay == n_lay - 1)
    def _():
        m_out[...] = m
        a_out[...] = dot(u, gate_ref[0]).astype(BF16)


def fwd_layers(x0, w_up, w_down, w_gate, first, n_lay, table, save_h, tile=512, chunk=1024):
    n_tok, dim = x0.shape
    ff = w_up.shape[2]
    last = n_lay - 1
    in_specs = [
        pl.BlockSpec((tile, dim), lambda l, t: (jnp.where(l == 0, t, n_tok // tile - 1), 0)),
        pl.BlockSpec((1, dim, ff), lambda l, t: (first + l, 0, 0)),
        pl.BlockSpec((1, ff, dim), lambda l, t: (first + l, 0, 0)),
        pl.BlockSpec((1, dim, dim), lambda l, t: (table, 0, 0)),
    ]
    end = pl.BlockSpec((tile, dim), lambda l, t: (jnp.where(l == last, t, 0), 0))
    out_specs = [pl.BlockSpec((1, tile, dim), lambda l, t: (l, t, 0))]
    out_shape = [jax.ShapeDtypeStruct((n_lay, n_tok, dim), BF16)]
    if save_h:
        out_specs.append(pl.BlockSpec((1, tile, ff), lambda l, t: (l, t, 0)))
        out_shape.append(jax.ShapeDtypeStruct((n_lay, n_tok, ff), BF16))
    out_specs += [end, end]
    out_shape += [jax.ShapeDtypeStruct((n_tok, dim), BF16)] * 2
    return pl.pallas_call(
        functools.partial(fwd_body, n_lay, tile, chunk, save_h),
        grid=(n_lay, n_tok // tile), in_specs=in_specs, out_specs=out_specs, out_shape=out_shape,
        scratch_shapes=[pltpu.VMEM((n_tok, dim), BF16)],
        compiler_params=params(60, ("arbitrary", "arbitrary")),
        cost_estimate=cost(n_lay * 4 * n_tok * dim * ff, n_lay * (4 * dim * ff + 2 * n_tok * ff)),
        name=f"fwd_{first}",
    )(x0, w_up, w_down, w_gate)


def bwd_body(n_lay, tile, chunk, c0_ref, x_ref, h_ref, up_ref, dn_ref, da_ref, gate_ref, cb_out, c_sc, du_sc):
    step, blk = pl.program_id(0), pl.program_id(1)
    rows = pl.ds(pl.multiple_of(blk * tile, tile), tile)

    @pl.when(step == 0)
    def _():
        c_sc[rows, :] = c0_ref[...].astype(F32)

    c_b = c_sc[rows, :].astype(BF16)
    acc = None
    for lo in range(0, up_ref.shape[2], chunk):
        d_act = dot(c_b, dn_ref[0, lo:lo + chunk, :], NT)
        d_h = (gelu_grad(h_ref[0, :, lo:lo + chunk].astype(F32)) * d_act).astype(BF16)
        part = dot(d_h, up_ref[0, :, lo:lo + chunk], NT)
        acc = part if acc is None else acc + part
    du_sc[...] = acc

    @pl.when(step == 0)
    def _():
        du_sc[...] += dot(da_ref[...], gate_ref[0], NT)

    x_f = x_ref[0].astype(F32)
    inv = lax.rsqrt(jnp.mean(x_f * x_f, axis=-1, keepdims=True) + EPS)
    du = du_sc[...]
    c_new = c_sc[rows, :] + (inv * du - x_f * (inv * inv * inv) * jnp.mean(x_f * du, axis=-1, keepdims=True))
    c_sc[rows, :] = c_new

    @pl.when(step == n_lay - 1)
    def _():
        cb_out[...] = c_new.astype(BF16)


def bwd_layers(c0, x_all, h_all, w_up, w_down, d_gate, w_gate, last_layer, table, tile=512, chunk=1024):
    n_lay, n_tok, dim = x_all.shape
    ff = w_up.shape[2]
    end_blk = n_tok // tile - 1
    first_only = pl.BlockSpec((tile, dim), lambda i, t: (jnp.where(i == 0, t, end_blk), 0))
    return pl.pallas_call(
        functools.partial(bwd_body, n_lay, tile, chunk),
        grid=(n_lay, n_tok // tile),
        in_specs=[
            first_only,
            pl.BlockSpec((1, tile, dim), lambda i, t: (n_lay - 1 - i, t, 0)),
            pl.BlockSpec((1, tile, ff), lambda i, t: (n_lay - 1 - i, t, 0)),
            pl.BlockSpec((1, dim, ff), lambda i, t: (last_layer - i, 0, 0)),
            pl.BlockSpec((1, ff, dim), lambda i, t: (last_layer - i, 0, 0)),
            first_only,
            pl.BlockSpec((1, dim, dim), lambda i, t: (table, 0, 0)),
        ],
        out_specs=pl.BlockSpec((tile, dim), lambda i, t: (jnp.where(i == n_lay - 1, t, 0), 0)),
        out_shape=jax.ShapeDtypeStruct((n_tok, dim), BF16),
        scratch_shapes=[pltpu.VMEM((n_tok, dim), F32), pltpu.VMEM((tile, dim), F32)],
        compiler_params=params(60, ("arbitrary", "arbitrary")),
        cost_estimate=cost(n_lay * 4 * n_tok * dim * ff, n_lay * (4 * dim * ff + 2 * n_tok * ff)),
        name="bwd",
    )(c0, x_all, h_all, w_up, w_down, d_gate, w_gate)


def mix_body(want_e, n_main, n_over, blk, extra_ref, ids_ref, slots_ref, main_ref, over_ref, more_ref, x_ref, m_ref, a_ref, proj_ref, x_out, *rest):
    if want_e:
        e_out, acc = rest
    else:
        (acc,) = rest
    keys = ids_ref[0]
    lo = n_main + n_over
    acc[...] = (dot((keys == slots_ref[0, :, :n_main]).astype(BF16), main_ref[...])
                + dot((keys == slots_ref[0, :, n_main:lo]).astype(BF16), over_ref[...]))

    @pl.loop(0, extra_ref[0])
    def _(i):
        at = pl.multiple_of(i * blk, blk)
        hit = (keys == slots_ref[0, :, pl.ds(lo + at, blk)]).astype(BF16)
        acc[...] += dot(hit, more_ref[pl.ds(at, blk), :])

    e_f = acc[...]
    g = gelu(a_ref[...].astype(F32)).astype(BF16).astype(F32)
    z = (g * e_f).astype(BF16)
    q = dot(z, proj_ref[0]).astype(BF16)
    x_out[...] = ((x_ref[0].astype(F32) + m_ref[...].astype(F32)) + q.astype(F32)).astype(BF16)
    if want_e:
        e_out[...] = e_f.astype(BF16)


def mix_rows(extra, ids, slots, main, over, more, x_all, m, a, w_proj, table, want_e, tile=512, blk=LANE):
    n_tok, dim = m.shape
    n_slot = slots.shape[2]
    last = x_all.shape[0] - 1
    tok = pl.BlockSpec((tile, dim), lambda t, *_: (t, 0))
    whole = lambda arr: pl.BlockSpec(arr.shape, lambda t, *_: (0, 0))
    outs = 2 if want_e else 1
    return pl.pallas_call(
        functools.partial(mix_body, want_e, main.shape[0], over.shape[0], blk),
        grid_spec=pltpu.PrefetchScalarGridSpec(
            num_scalar_prefetch=1, grid=(n_tok // tile,),
            in_specs=[
                pl.BlockSpec((1, tile, 1), lambda t, *_: (table, t, 0)),
                pl.BlockSpec((1, 1, n_slot), lambda t, *_: (table, 0, 0)),
                whole(main), whole(over), whole(more),
                pl.BlockSpec((1, tile, dim), lambda t, *_: (last, t, 0)),
                tok, tok,
                pl.BlockSpec((1, dim, dim), lambda t, *_: (table, 0, 0)),
            ],
            out_specs=[tok] * outs,
            scratch_shapes=[pltpu.VMEM((tile, dim), F32)],
        ),
        out_shape=[jax.ShapeDtypeStruct((n_tok, dim), BF16)] * outs,
        compiler_params=params(48, ("arbitrary",)),
        cost_estimate=cost(2 * n_tok * dim * (dim + 1408), 12 * n_tok * dim),
        name=f"mix_{table}",
    )(extra, ids, slots, main, over, more, x_all, m, a, w_proj)


def grad_body(steps, tile, want_da, extra_ref, ids_ref, slots_ref, c_ref, a_ref, proj_ref, *rest):
    if want_da:
        e_ref, main_out, over_out, more_out, da_out, hi_sc, mid_sc, lo_sc = rest
    else:
        main_out, over_out, more_out, hi_sc, mid_sc, lo_sc = rest
    step = pl.program_id(0)
    main_steps, more_blk = steps
    n_main, n_over = main_out.shape[0] * main_steps, over_out.shape[0]

    @pl.when(step == 0)
    def _():
        @pl.loop(0, c_ref.shape[0], step=tile)
        def _(lo):
            rows = pl.ds(pl.multiple_of(lo, tile), tile)
            dz = dot(c_ref[rows, :], proj_ref[0], NT)
            a_f = a_ref[rows, :].astype(F32)
            g = gelu(a_f).astype(BF16).astype(F32)
            if want_da:
                da_out[rows, :] = (gelu_grad(a_f) * (dz * e_ref[rows, :].astype(F32))).astype(BF16)
            grad = g * dz
            hi = grad.astype(BF16)
            left = grad - hi.astype(F32)
            mid = left.astype(BF16)
            hi_sc[rows, :] = hi
            mid_sc[rows, :] = mid
            lo_sc[rows, :] = (left - mid.astype(F32)).astype(BF16)

    def sums(first, size):
        hit = (slots_ref[0, pl.ds(first, size), :] == ids_ref[0]).astype(BF16)
        return (dot(hit, lo_sc[...]) + dot(hit, mid_sc[...])) + dot(hit, hi_sc[...])

    @pl.when(step < main_steps)
    def _():
        blk = main_out.shape[0]
        main_out[...] = sums(pl.multiple_of(step * blk, blk), blk)

    @pl.when(step == main_steps)
    def _():
        over_out[...] = sums(n_main, n_over)

    @pl.when((step > main_steps) & ((step - main_steps - 1) < extra_ref[0]))
    def _():
        more_out[...] = sums(pl.multiple_of(n_main + n_over + (step - main_steps - 1) * more_blk, more_blk), more_blk)


def grad_rows(extra, ids, slots, c_b, a, e, w_proj, table, n_main, n_over, tile=512, main_steps=2, more_blk=LANE):
    n_tok, dim = c_b.shape
    n_slot = slots.shape[1]
    n_more = n_slot - n_main - n_over
    want_da = e is not None
    whole = pl.BlockSpec((n_tok, dim), lambda s, *_: (0, 0))
    in_specs = [
        pl.BlockSpec((1, 1, n_tok), lambda s, *_: (table, 0, 0)),
        pl.BlockSpec((1, n_slot, 1), lambda s, *_: (table, 0, 0)),
        whole, whole,
        pl.BlockSpec((1, dim, dim), lambda s, *_: (table, 0, 0)),
    ]

    def more_at(s, extra_ref):
        return (jnp.clip(s - main_steps - 1, 0, jnp.maximum(extra_ref[0] - 1, 0)), 0)

    out_specs = [
        pl.BlockSpec((n_main // main_steps, dim), lambda s, *_: (jnp.minimum(s, main_steps - 1), 0)),
        pl.BlockSpec((n_over, dim), lambda s, *_: (0, 0)),
        pl.BlockSpec((more_blk, dim), more_at),
    ]
    out_shape = [jax.ShapeDtypeStruct((n, dim), F32) for n in (n_main, n_over, n_more)]
    args = [extra, ids, slots, c_b, a, w_proj]
    if want_da:
        in_specs.append(whole)
        out_specs.append(whole)
        out_shape.append(jax.ShapeDtypeStruct((n_tok, dim), BF16))
        args.append(e)
    return pl.pallas_call(
        functools.partial(grad_body, (main_steps, more_blk), tile, want_da),
        grid_spec=pltpu.PrefetchScalarGridSpec(
            num_scalar_prefetch=1, grid=(main_steps + 1 + n_more // more_blk,), in_specs=in_specs, out_specs=out_specs,
            scratch_shapes=[pltpu.VMEM((n_tok, dim), BF16)] * 3,
        ),
        out_shape=out_shape,
        compiler_params=params(60, ("arbitrary",)),
        cost_estimate=cost(2 * n_tok * dim * (dim + 3 * 1408), 12 * n_tok * dim),
        name=f"grad_{table}",
    )(*args)


def local_row(key, base, rows_dev):
    row = key - base
    return jnp.where((row >= 0) & (row < rows_dev), row, rows_dev)


def unflatten(flat_sc, tab_ref, rows_dev, parts):
    @pl.loop(0, rows_dev // UNIT)
    def _(i):
        block = tab_ref[0, pl.ds(pl.multiple_of(i * UNIT, UNIT), UNIT), :].astype(F32)
        for p in range(parts):
            flat_sc[pl.ds(i * (UNIT * parts) + p, UNIT, stride=parts), :] = block[:, p * LANE:(p + 1) * LANE]


def pick_unit(slots_ref, src, at, base, rows_dev, parts, flat_sc, stage_sc, out_ref, to):
    for k in range(UNIT):
        row = local_row(slots_ref[src, at + k], base, rows_dev)
        stage_sc[k * parts:(k + 1) * parts, :] = flat_sc[pl.ds(row * parts, parts), :]
    rows = pl.ds(pl.multiple_of(to, UNIT), UNIT)
    for p in range(parts):
        out_ref[rows, p * LANE:(p + 1) * LANE] = stage_sc[pl.ds(p, UNIT, stride=parts), :].astype(BF16)


def serve_body(n_dev, rows_dev, parts, spans, meta_ref, slots_ref, tab_ref, *rest):
    outs, (flat_sc, stage_sc) = rest[:len(spans)], rest[len(spans):]
    me = meta_ref[0]
    base = me * rows_dev
    unflatten(flat_sc, tab_ref, rows_dev, parts)
    flat_sc[rows_dev * parts:(rows_dev + 1) * parts, :] = jnp.zeros((parts, LANE), F32)
    for out_ref, (first, size, direct) in zip(outs, spans):
        if not direct:
            @pl.loop(0, n_dev * size, step=UNIT)
            def _(i):
                out_ref[pl.ds(pl.multiple_of(i, UNIT), UNIT), :] = jnp.zeros((UNIT, parts * LANE), BF16)

        for src in range(n_dev):
            if direct:
                begin, end, at = 0, size // UNIT, first + me * size
            else:
                begin = jnp.clip((meta_ref[1 + src] - (first - n_dev * MAIN)) // UNIT, 0, size // UNIT)
                end = jnp.clip((meta_ref[1 + n_dev + src] - (first - n_dev * MAIN) + (UNIT - 1)) // UNIT, 0, size // UNIT)
                at = first

            @pl.loop(begin, end)
            def _(i):
                pick_unit(slots_ref, src, at + i * UNIT, base, rows_dev, parts, flat_sc, stage_sc, out_ref, src * size + i * UNIT)


def serve_rows(meta, slots_all, tables, table, n_dev, spans):
    _, rows_dev, dim = tables.shape
    parts = dim // LANE
    sizes = [n_dev * size for _, size, _ in spans]
    return pl.pallas_call(
        functools.partial(serve_body, n_dev, rows_dev, parts, spans),
        grid_spec=pltpu.PrefetchScalarGridSpec(
            num_scalar_prefetch=2, grid=(1,),
            in_specs=[pl.BlockSpec((1, rows_dev, dim), lambda i, *_: (table, 0, 0), pipeline_mode=pl.Buffered(1))],
            out_specs=[pl.BlockSpec((n, dim), lambda i, *_: (0, 0), pipeline_mode=pl.Buffered(1)) for n in sizes],
            scratch_shapes=[pltpu.VMEM(((rows_dev + 8) * parts, LANE), F32), pltpu.VMEM((UNIT * parts, LANE), F32)],
        ),
        out_shape=[jax.ShapeDtypeStruct((n, dim), BF16) for n in sizes],
        compiler_params=params(62, ("arbitrary",)),
        cost_estimate=cost(20e9, 22e6),
        name=f"serve_{table}",
    )(meta, slots_all, tables)


def collect_body(n_dev, rows_dev, parts, sizes, has_prev, meta_ref, slots_ref, main_ref, over_ref, more_ref, *rest):
    if has_prev:
        rest = rest[1:]
    out_ref, flat_sc, main_sc, over_sc, unit_sc, stage_sc, sems = rest
    step = pl.program_id(0)
    me = meta_ref[0]
    base = me * rows_dev
    n_main, n_over, n_more = sizes

    def part_copy(src, dst, i, n, sem):
        rows = pl.ds(i * n, n)
        return pltpu.make_async_copy(src.at[rows, :], dst.at[rows, :], sem)

    def add_unit(src, at, buf, rows):
        for p in range(parts):
            stage_sc[pl.ds(p, UNIT, stride=parts), :] = buf[rows, p * LANE:(p + 1) * LANE]
        where = [pl.ds(local_row(slots_ref[src, at + k], base, rows_dev) * parts, parts) for k in range(UNIT)]
        sums = [flat_sc[where[k], :] + stage_sc[k * parts:(k + 1) * parts, :] for k in range(UNIT)]
        for k in range(UNIT):
            flat_sc[where[k], :] = sums[k]

    def units(src, first, size):
        begin = jnp.clip((meta_ref[1 + src] - first) // UNIT, 0, size // UNIT)
        end = jnp.clip((meta_ref[1 + n_dev + src] - first + (UNIT - 1)) // UNIT, 0, size // UNIT)
        return begin, end

    @pl.when(step == 0)
    def _():
        for s in range(n_dev):
            part_copy(main_ref, main_sc, s, n_main, sems.at[s]).start()
            part_copy(over_ref, over_sc, s, n_over, sems.at[n_dev + s]).start()

        @pl.loop(0, rows_dev // 8)
        def _(i):
            flat_sc[pl.ds(pl.multiple_of(i * 8 * parts, 8), 8 * parts), :] = jnp.zeros((8 * parts, LANE), F32)

        for s in range(n_dev):
            part_copy(main_ref, main_sc, s, n_main, sems.at[s]).wait()

            @pl.loop(0, (meta_ref[1 + 2 * n_dev + s] + (UNIT - 1)) // UNIT)
            def _(i):
                add_unit(s, me * n_main + i * UNIT, main_sc, pl.ds(pl.multiple_of(s * n_main + i * UNIT, UNIT), UNIT))

        for s in range(n_dev):
            part_copy(over_ref, over_sc, s, n_over, sems.at[n_dev + s]).wait()

            @pl.loop(*units(s, 0, n_over))
            def _(i):
                add_unit(s, n_dev * n_main + i * UNIT, over_sc, pl.ds(pl.multiple_of(s * n_over + i * UNIT, UNIT), UNIT))

        for s in range(n_dev):
            @pl.loop(*units(s, n_over, n_more))
            def _(i):
                rows = pl.ds(pl.multiple_of(s * n_more + i * UNIT, UNIT), UNIT)
                copy = pltpu.make_async_copy(more_ref.at[rows, :], unit_sc, sems.at[2 * n_dev])
                copy.start()
                copy.wait()
                add_unit(s, n_dev * n_main + n_over + i * UNIT, unit_sc, pl.ds(0, UNIT))

    @pl.when(step > 0)
    def _():
        blk = out_ref.shape[1]
        first = (step - 1) * (blk * parts)

        @pl.loop(0, blk // 8)
        def _(i):
            to = pl.ds(pl.multiple_of(i * 8, 8), 8)
            for p in range(parts):
                out_ref[0, to, p * LANE:(p + 1) * LANE] = flat_sc[pl.ds(first + i * (8 * parts) + p, 8, stride=parts), :]


def collect_rows(meta, slots_all, main, over, more, prev, table, n_tables, rows_dev, n_dev, n_blk=6):
    dim = main.shape[1]
    parts = dim // LANE
    blk = rows_dev // n_blk
    any_spec = pl.BlockSpec(memory_space=pl.ANY)
    args = [meta, slots_all, main, over, more]
    alias = {}
    if prev is not None:
        args.append(prev)
        alias = {5: 0}
    return pl.pallas_call(
        functools.partial(collect_body, n_dev, rows_dev, parts, [r.shape[0] // n_dev for r in (main, over, more)], prev is not None),
        grid_spec=pltpu.PrefetchScalarGridSpec(
            num_scalar_prefetch=2, grid=(1 + n_blk,), in_specs=[any_spec] * (len(args) - 2),
            out_specs=pl.BlockSpec((1, blk, dim), lambda i, *_: (table, jnp.maximum(i - 1, 0), 0)),
            scratch_shapes=[
                pltpu.VMEM(((rows_dev + 8) * parts, LANE), F32),
                pltpu.VMEM(main.shape, F32),
                pltpu.VMEM(over.shape, F32),
                pltpu.VMEM((UNIT, dim), F32),
                pltpu.VMEM((UNIT * parts, LANE), F32),
                pltpu.SemaphoreType.DMA((2 * n_dev + 1,)),
            ],
        ),
        out_shape=jax.ShapeDtypeStruct((n_tables, rows_dev, dim), F32),
        input_output_aliases=alias,
        compiler_params=params(56, ("arbitrary",)),
        cost_estimate=cost(20e9, 30e6),
        name=f"collect_{table}",
    )(*args)


def blank(shape, dtype):
    return pl.pallas_call(lambda o: None, out_specs=pl.BlockSpec(memory_space=pl.ANY),
                          out_shape=jax.ShapeDtypeStruct(shape, dtype), name="blank")()


def layout_body(n_dev, cnt_ref, uniq_ref, out_ref):
    n_tab, _, n = uniq_ref.shape
    n_main = n_dev * MAIN
    lane = lax.broadcasted_iota(jnp.int32, (1, n), 1)
    small = lax.broadcasted_iota(jnp.int32, (1, MAIN), 1)
    for j in range(n_tab):
        uniq = uniq_ref[j]
        over = jnp.full((1, n), -1, jnp.int32)
        tail = jnp.zeros((1, LANE), jnp.int32)
        start = jnp.int32(0)
        at = jnp.int32(0)
        for o in range(n_dev):
            cnt = cnt_ref[j, o]
            head = pltpu.roll(uniq, lax.rem(n - start, n), 1)[:, :MAIN]
            out_ref[j, :, o * MAIN:(o + 1) * MAIN] = jnp.where(small < cnt, head, -1)
            extra = jnp.maximum(cnt - MAIN, 0)
            moved = pltpu.roll(uniq, lax.rem(2 * n + at - start - MAIN, n), 1)
            over = jnp.where((lane >= at) & (lane < at + extra), moved, over)
            tail = jnp.where(lax.broadcasted_iota(jnp.int32, (1, LANE), 1) == o, cnt, tail)
            start = start + cnt
            at = at + extra
        out_ref[j, :, n_main:n_main + n] = over
        out_ref[j, :, n_main + n:] = tail


def route(ids, rows_dev, n_dev):
    n_tab, n_tok = ids.shape
    ordered = lax.sort(ids, dimension=1)
    first = jnp.concatenate([jnp.ones((n_tab, 1), bool), ordered[:, 1:] != ordered[:, :-1]], axis=1)
    lo = (jnp.arange(n_dev, dtype=jnp.int32) * rows_dev)[None, :, None]
    mine = first[:, None, :] & (ordered[:, None, :] >= lo) & (ordered[:, None, :] < lo + rows_dev)
    counts = jnp.sum(mine.astype(jnp.int32), axis=2)
    uniq = lax.sort(jnp.where(first, ordered, jnp.int32(2 ** 30)), dimension=1)
    return pl.pallas_call(
        functools.partial(layout_body, n_dev),
        grid_spec=pltpu.PrefetchScalarGridSpec(
            num_scalar_prefetch=1, grid=(1,),
            in_specs=[pl.BlockSpec((n_tab, 1, n_tok), lambda i, *_: (0, 0, 0))],
            out_specs=pl.BlockSpec((n_tab, 1, n_dev * MAIN + n_tok + LANE), lambda i, *_: (0, 0, 0))),
        out_shape=jax.ShapeDtypeStruct((n_tab, 1, n_dev * MAIN + n_tok + LANE), jnp.int32),
        name="layout",
    )(counts, uniq.reshape(n_tab, 1, n_tok))


def solution(mesh):
    n_dev = mesh.shape['emb']
    tok_spec = P('emb', None)
    tab_spec = P(None, 'emb', None)

    def local_program(x_start, d_out, token_ids, w_up, w_down, w_gate, w_proj, tables):
        n_tab, n_tok = token_ids.shape[:2]
        rows_dev, dim = tables.shape[1:]
        layers = w_up.shape[0]
        me = lax.axis_index('emb').astype(jnp.int32)
        ids = token_ids.reshape(n_tab, n_tok)
        sent = route(ids, rows_dev, n_dev)
        n_main, n_over, n_more = n_dev * MAIN, OVER, n_tok - OVER
        n_slot = n_main + n_tok
        got = lax.all_gather(sent[:, 0], 'emb')
        counts = got[:, :, n_slot:n_slot + n_dev]
        extra = jnp.maximum(counts - MAIN, 0)
        starts = jnp.cumsum(extra, axis=2) - extra
        rest = jnp.sum(extra, axis=2)
        ids_col, ids_row = token_ids, ids.reshape(n_tab, 1, n_tok)
        slots_row = sent[:, :, :n_slot]
        slots_col = slots_row.reshape(n_tab, n_slot, 1)
        plan = []
        for j in range(n_tab):
            to_me = lambda a: lax.dynamic_index_in_dim(a[:, j], me, axis=1, keepdims=False)
            begin = to_me(starts)
            meta = jnp.concatenate([me[None], begin, begin + to_me(extra), jnp.minimum(to_me(counts), MAIN)])
            mine = lax.dynamic_index_in_dim(rest[:, j], me, axis=0, keepdims=True)
            more = jnp.maximum(mine - OVER + (LANE - 1), 0) // LANE
            plan.append(dict(meta=meta, slots=got[:, j, :n_slot], more=more, spill=jnp.any(rest[:, j] > OVER)))

        def fetch(j):
            p = plan[j]
            main, over = serve_rows(p['meta'], p['slots'], tables, j, n_dev, ((0, MAIN, True), (n_main, OVER, False)))
            main = lax.all_to_all(main, 'emb', 0, 0, tiled=True)
            over = lax.psum_scatter(over, 'emb', scatter_dimension=0, tiled=True)

            def all_rows():
                (more,) = serve_rows(p['meta'], p['slots'], tables, j, n_dev, ((n_main + OVER, n_more, False),))
                return lax.psum_scatter(more, 'emb', scatter_dimension=0, tiled=True)

            more = lax.cond(p['spill'], all_rows, lambda: blank((n_more, dim), BF16))
            return main, over, more

        def give_back(j, main, over, more):
            main = lax.all_to_all(main, 'emb', 0, 0, tiled=True)
            over = lax.all_gather(over, 'emb', axis=0, tiled=True)
            more = lax.cond(plan[j]['spill'], lambda: lax.all_gather(more, 'emb', axis=0, tiled=True),
                            lambda: blank((n_dev * n_more, dim), F32))
            return main, over, more

        def collect(j, received, prev):
            return collect_rows(plan[j]['meta'], plan[j]['slots'], *received, prev, j, n_tab, rows_dev, n_dev)

        rows_0 = fetch(0)
        rows_1 = fetch(1)
        x_a, m_a, a_0 = fwd_layers(x_start, w_up, w_down, w_gate, 0, 2, 0, False)
        (x_2,) = mix_rows(plan[0]['more'], ids_col, slots_row, *rows_0, x_a, m_a, a_0, w_proj, 0, False)
        x_b, h_b, m_b, a_1 = fwd_layers(x_2, w_up, w_down, w_gate, 2, layers - 2, 1, True)
        x_end, e_1 = mix_rows(plan[1]['more'], ids_col, slots_row, *rows_1, x_b, m_b, a_1, w_proj, 1, True)
        *sums_1, d_a = grad_rows(plan[1]['more'], ids_row, slots_col, d_out, a_1, e_1, w_proj, 1, n_main, n_over)
        recv_1 = give_back(1, *sums_1)
        c_b = bwd_layers(d_out, x_b, h_b, w_up, w_down, d_a, w_gate, layers - 1, 1)
        sums_0 = grad_rows(plan[0]['more'], ids_row, slots_col, c_b, a_0, None, w_proj, 0, n_main, n_over)
        recv_0 = give_back(0, *sums_0)
        grads = collect(0, recv_0, collect(1, recv_1, None))
        return x_end, grads

    return jax.shard_map(local_program, mesh=mesh, in_specs=(tok_spec, tok_spec, tab_spec, P(), P(), P(), P(), tab_spec), out_specs=(tok_spec, tab_spec), check_vma=False)
```

```python
import functools

import jax
import jax.numpy as jnp
from jax import lax
from jax.experimental import pallas as pl
from jax.experimental.pallas import tpu as pltpu
from jax.sharding import PartitionSpec as P

EPS = 1e-6
GELU_K = 0.7978845608028654
GELU_C = 0.044715
F32 = jnp.float32
BF16 = jnp.bfloat16
UNIT = 16
LANE = 128
SUB = 256
MAIN = 128
OVER = 320
OVER_SLOTS = 384
NT = (((1,), (1,)), ((), ()))
NN = (((1,), (0,)), ((), ()))


def dot(a, b, dims=NN):
    return lax.dot_general(a, b, dims, preferred_element_type=F32)


def gelu(v):
    half = 0.5 * v
    return half + half * jnp.tanh(v * (GELU_K + (GELU_K * GELU_C) * (v * v)))


def gelu_grad(v):
    sq = v * v
    th = jnp.tanh(v * (GELU_K + (GELU_K * GELU_C) * sq))
    return (0.5 + 0.5 * th) * (1.0 + (v * (GELU_K + (3.0 * GELU_K * GELU_C) * sq)) * (1.0 - th))


def params(mb, sem=None):
    return pltpu.CompilerParams(vmem_limit_bytes=mb * 1024 * 1024, dimension_semantics=sem)


def cost(flops, nbytes):
    return pl.CostEstimate(flops=int(flops), bytes_accessed=int(nbytes), transcendentals=0)


def fwd_body(n_lay, tile, chunk, save_h, x0_ref, up_ref, dn_ref, gate_ref, *rest):
    if save_h:
        x_out, h_out, a_out, x_sc = rest
    else:
        x_out, m_out, a_out, x_sc = rest
    lay, blk = pl.program_id(0), pl.program_id(1)
    rows = pl.ds(pl.multiple_of(blk * tile, tile), tile)

    @pl.when(lay == 0)
    def _():
        x_sc[rows, :] = x0_ref[...]

    x_bf = x_sc[rows, :]
    x_out[0] = x_bf
    x_f = x_bf.astype(F32)
    inv = lax.rsqrt(jnp.mean(x_f * x_f, axis=-1, keepdims=True) + EPS)
    u = (x_f * inv).astype(BF16)
    sub = min(tile, SUB)
    ff = up_ref.shape[2]
    todo = [(r, lo) for r in range(0, tile, sub) for lo in range(0, ff, chunk)]
    up_dot = lambda r, lo: dot(u[r:r + sub, :], up_ref[0, :, lo:lo + chunk])

    def mlp():
        nxt = up_dot(*todo[0])
        accs = {}
        for i, (r, lo) in enumerate(todo):
            h = nxt.astype(BF16)
            if i + 1 < len(todo):
                nxt = up_dot(*todo[i + 1])
            if save_h:
                h_out[0, r:r + sub, lo:lo + chunk] = h
            act = gelu(h.astype(F32)).astype(BF16)
            part = dot(act, dn_ref[0, lo:lo + chunk, :])
            accs[r] = part if lo == 0 else accs[r] + part
        return jnp.concatenate([accs[r].astype(BF16) for r in sorted(accs)], axis=0)

    if save_h:
        @pl.when(lay < n_lay - 1)
        def _():
            x_sc[rows, :] = (x_f + mlp().astype(F32)).astype(BF16)

        @pl.when(lay == n_lay - 1)
        def _():
            h_out[0] = dot(u, up_ref[0]).astype(BF16)
    else:
        m = mlp()
        x_sc[rows, :] = (x_f + m.astype(F32)).astype(BF16)

    @pl.when(lay == n_lay - 1)
    def _():
        if not save_h:
            m_out[...] = m
        a_out[...] = dot(u, gate_ref[0]).astype(BF16)


def fwd_layers(x0, w_up, w_down, w_gate, first, n_lay, table, save_h, tile=512, chunk=3072):
    n_tok, dim = x0.shape
    ff = w_up.shape[2]
    last = n_lay - 1
    in_specs = [
        pl.BlockSpec((tile, dim), lambda l, t: (jnp.where(l == 0, t, n_tok // tile - 1), 0)),
        pl.BlockSpec((1, dim, ff), lambda l, t: (first + l, 0, 0)),
        pl.BlockSpec((1, ff, dim), lambda l, t: (first + l, 0, 0)),
        pl.BlockSpec((1, dim, dim), lambda l, t: (table, 0, 0)),
    ]
    end = pl.BlockSpec((tile, dim), lambda l, t: (jnp.where(l == last, t, 0), 0))
    out_specs = [pl.BlockSpec((1, tile, dim), lambda l, t: (l, t, 0))]
    out_shape = [jax.ShapeDtypeStruct((n_lay, n_tok, dim), BF16)]
    if save_h:
        out_specs.append(pl.BlockSpec((1, tile, ff), lambda l, t: (l, t, 0)))
        out_shape.append(jax.ShapeDtypeStruct((n_lay, n_tok, ff), BF16))
    n_end = 1 if save_h else 2
    out_specs += [end] * n_end
    out_shape += [jax.ShapeDtypeStruct((n_tok, dim), BF16)] * n_end
    return pl.pallas_call(
        functools.partial(fwd_body, n_lay, tile, chunk, save_h),
        grid=(n_lay, n_tok // tile), in_specs=in_specs, out_specs=out_specs, out_shape=out_shape,
        scratch_shapes=[pltpu.VMEM((n_tok, dim), BF16)],
        compiler_params=params(60, ("arbitrary", "arbitrary")),
        cost_estimate=cost(n_lay * 4 * n_tok * dim * ff, n_lay * (4 * dim * ff + 2 * n_tok * ff)),
        name=f"fwd_{first}",
    )(x0, w_up, w_down, w_gate)


def bwd_body(n_lay, tile, chunk, c0_ref, x_ref, h_ref, up_ref, dn_ref, da_ref, gate_ref, cb_out, c_sc, du_sc):
    step, blk = pl.program_id(0), pl.program_id(1)
    rows = pl.ds(pl.multiple_of(blk * tile, tile), tile)

    @pl.when(step == 0)
    def _():
        c_sc[rows, :] = c0_ref[...].astype(F32)

    c_b = c_sc[rows, :].astype(BF16)
    sub = tile
    ff = up_ref.shape[2]
    todo = [(r, lo) for r in range(0, tile, sub) for lo in range(0, ff, chunk)]
    act_dot = lambda r, lo: dot(c_b[r:r + sub, :], dn_ref[0, lo:lo + chunk, :], NT)
    nxt = act_dot(*todo[0])
    for i, (r, lo) in enumerate(todo):
        d_act = nxt
        if i + 1 < len(todo):
            nxt = act_dot(*todo[i + 1])
        d_h = (gelu_grad(h_ref[0, r:r + sub, lo:lo + chunk].astype(F32)) * d_act).astype(BF16)
        part = dot(d_h, up_ref[0, :, lo:lo + chunk], NT)
        if lo == 0:
            du_sc[r:r + sub, :] = part
        else:
            du_sc[r:r + sub, :] += part

    @pl.when(step == 0)
    def _():
        du_sc[...] += dot(da_ref[...], gate_ref[0], NT)

    x_f = x_ref[0].astype(F32)
    inv = lax.rsqrt(jnp.mean(x_f * x_f, axis=-1, keepdims=True) + EPS)
    du = du_sc[...]
    c_new = c_sc[rows, :] + (inv * du - x_f * (inv * inv * inv) * jnp.mean(x_f * du, axis=-1, keepdims=True))
    c_sc[rows, :] = c_new

    @pl.when(step == n_lay - 1)
    def _():
        cb_out[...] = c_new.astype(BF16)


def bwd_layers(c0, x_all, h_all, w_up, w_down, d_gate, w_gate, last_layer, table, tile=512, chunk=1536):
    n_lay, n_tok, dim = x_all.shape
    ff = w_up.shape[2]
    end_blk = n_tok // tile - 1
    first_only = pl.BlockSpec((tile, dim), lambda i, t: (jnp.where(i == 0, t, end_blk), 0))
    return pl.pallas_call(
        functools.partial(bwd_body, n_lay, tile, chunk),
        grid=(n_lay, n_tok // tile),
        in_specs=[
            first_only,
            pl.BlockSpec((1, tile, dim), lambda i, t: (n_lay - 1 - i, t, 0)),
            pl.BlockSpec((1, tile, ff), lambda i, t: (n_lay - 1 - i, t, 0)),
            pl.BlockSpec((1, dim, ff), lambda i, t: (last_layer - i, 0, 0)),
            pl.BlockSpec((1, ff, dim), lambda i, t: (last_layer - i, 0, 0)),
            first_only,
            pl.BlockSpec((1, dim, dim), lambda i, t: (table, 0, 0)),
        ],
        out_specs=pl.BlockSpec((tile, dim), lambda i, t: (jnp.where(i == n_lay - 1, t, 0), 0)),
        out_shape=jax.ShapeDtypeStruct((n_tok, dim), BF16),
        scratch_shapes=[pltpu.VMEM((n_tok, dim), F32), pltpu.VMEM((tile, dim), F32)],
        compiler_params=params(60, ("arbitrary", "arbitrary")),
        cost_estimate=cost(n_lay * 4 * n_tok * dim * ff, n_lay * (4 * dim * ff + 2 * n_tok * ff)),
        name="bwd",
    )(c0, x_all, h_all, w_up, w_down, d_gate, w_gate)


def expand(n_main, n_over, blk, extra_ref, ids_ref, slots_ref, main_ref, over_ref, more_ref, acc):
    keys = ids_ref[0]
    lo = n_main + OVER_SLOTS
    acc[...] = (dot((keys == slots_ref[0, :, :n_main]).astype(BF16), main_ref[...])
                + dot((keys == slots_ref[0, :, n_main:n_main + n_over]).astype(BF16), over_ref[...]))

    @pl.loop(0, extra_ref[0])
    def _(i):
        at = pl.multiple_of(i * blk, blk)
        hit = (keys == slots_ref[0, :, pl.ds(lo + at, blk)]).astype(BF16)
        acc[...] += dot(hit, more_ref[pl.ds(at, blk), :])

    return acc[...]


def gated(a_ref, e_f, proj_ref):
    g = gelu(a_ref[...].astype(F32)).astype(BF16).astype(F32)
    return dot((g * e_f).astype(BF16), proj_ref[0]).astype(BF16).astype(F32)


def mix_body(n_main, n_over, blk, extra_ref, ids_ref, slots_ref, main_ref, over_ref, more_ref, x_ref, m_ref, a_ref, proj_ref, x_out, acc):
    e_f = expand(n_main, n_over, blk, extra_ref, ids_ref, slots_ref, main_ref, over_ref, more_ref, acc)
    q = gated(a_ref, e_f, proj_ref)
    x_out[...] = ((x_ref[0].astype(F32) + m_ref[...].astype(F32)) + q).astype(BF16)


def expand_body(n_main, n_over, blk, extra_ref, ids_ref, slots_ref, main_ref, over_ref, more_ref, e_out, acc):
    e_out[...] = expand(n_main, n_over, blk, extra_ref, ids_ref, slots_ref, main_ref, over_ref, more_ref, acc).astype(BF16)


def mix_rows(extra, ids, slots, main, over, more, layer_args, w_proj, table, tile=512, blk=LANE):
    n_tok, dim = ids.shape[1], main.shape[1]
    n_slot = slots.shape[2]
    tok = pl.BlockSpec((tile, dim), lambda t, *_: (t, 0))
    whole = lambda arr: pl.BlockSpec(arr.shape, lambda t, *_: (0, 0))
    in_specs = [
        pl.BlockSpec((1, tile, 1), lambda t, *_: (table, t, 0)),
        pl.BlockSpec((1, 1, n_slot), lambda t, *_: (table, 0, 0)),
        whole(main), whole(over), whole(more),
    ]
    args = [extra, ids, slots, main, over, more]
    if layer_args is not None:
        last = layer_args[0].shape[0] - 1
        in_specs += [
            pl.BlockSpec((1, tile, dim), lambda t, *_: (last, t, 0)), tok, tok,
            pl.BlockSpec((1, dim, dim), lambda t, *_: (table, 0, 0)),
        ]
        args += [*layer_args, w_proj]
    return pl.pallas_call(
        functools.partial(expand_body if layer_args is None else mix_body, main.shape[0], over.shape[0], blk),
        grid_spec=pltpu.PrefetchScalarGridSpec(
            num_scalar_prefetch=1, grid=(n_tok // tile,), in_specs=in_specs, out_specs=tok,
            scratch_shapes=[pltpu.VMEM((tile, dim), F32)],
        ),
        out_shape=jax.ShapeDtypeStruct((n_tok, dim), BF16),
        compiler_params=params(48, ("arbitrary",)),
        cost_estimate=cost(2 * n_tok * dim * (dim + 1344), 12 * n_tok * dim),
        name=f"mix_{table}",
    )(*args)


def finish_body(chunk, after_ref, x_ref, h_ref, a_ref, e_ref, dn_ref, proj_ref, x_out):
    del after_ref
    q = gated(a_ref, e_ref[...].astype(F32), proj_ref)
    acc = None
    for lo in range(0, h_ref.shape[2], chunk):
        act = gelu(h_ref[0, :, lo:lo + chunk].astype(F32)).astype(BF16)
        part = dot(act, dn_ref[0, lo:lo + chunk, :])
        acc = part if acc is None else acc + part
    x_out[...] = ((x_ref[0].astype(F32) + acc.astype(BF16).astype(F32)) + q).astype(BF16)


def finish(after, x_all, h_all, a, e, w_down, w_proj, layer, table, tile=512, chunk=1024):
    n_lay, n_tok, dim = x_all.shape
    ff = h_all.shape[2]
    tok = pl.BlockSpec((tile, dim), lambda t: (t, 0))
    return pl.pallas_call(
        functools.partial(finish_body, chunk),
        grid=(n_tok // tile,),
        in_specs=[
            pl.BlockSpec(memory_space=pl.ANY),
            pl.BlockSpec((1, tile, dim), lambda t: (n_lay - 1, t, 0)),
            pl.BlockSpec((1, tile, ff), lambda t: (n_lay - 1, t, 0)),
            tok, tok,
            pl.BlockSpec((1, ff, dim), lambda t: (layer, 0, 0)),
            pl.BlockSpec((1, dim, dim), lambda t: (table, 0, 0)),
        ],
        out_specs=tok,
        out_shape=jax.ShapeDtypeStruct((n_tok, dim), BF16),
        compiler_params=params(48, ("arbitrary",)),
        cost_estimate=cost(2 * n_tok * dim * (dim + ff), 6 * n_tok * dim + 2 * n_tok * ff),
        name="finish",
    )(after, x_all, h_all, a, e, w_down, w_proj)


def grad_body(steps, tile, want_da, n_after, extra_ref, ids_ref, slots_ref, c_ref, a_ref, proj_ref, *rest):
    rest = rest[n_after:]
    if want_da:
        e_ref, main_out, over_out, more_out, da_out, hi_sc, mid_sc, lo_sc = rest
    else:
        main_out, over_out, more_out, hi_sc, mid_sc, lo_sc = rest
    step = pl.program_id(0)
    main_steps, more_blk = steps
    n_main, n_over = main_out.shape[0] * main_steps, over_out.shape[0]

    @pl.when(step == 0)
    def _():
        @pl.loop(0, c_ref.shape[0], step=tile)
        def _(lo):
            rows = pl.ds(pl.multiple_of(lo, tile), tile)
            dz = dot(c_ref[rows, :], proj_ref[0], NT)
            a_f = a_ref[rows, :].astype(F32)
            g = gelu(a_f).astype(BF16).astype(F32)
            if want_da:
                da_out[rows, :] = (gelu_grad(a_f) * (dz * e_ref[rows, :].astype(F32))).astype(BF16)
            grad = g * dz
            hi = grad.astype(BF16)
            left = grad - hi.astype(F32)
            mid = left.astype(BF16)
            hi_sc[rows, :] = hi
            mid_sc[rows, :] = mid
            lo_sc[rows, :] = (left - mid.astype(F32)).astype(BF16)

    def sums(first, size):
        hit = (slots_ref[0, pl.ds(first, size), :] == ids_ref[0]).astype(BF16)
        return (dot(hit, lo_sc[...]) + dot(hit, mid_sc[...])) + dot(hit, hi_sc[...])

    @pl.when(step < main_steps)
    def _():
        blk = main_out.shape[0]
        main_out[...] = sums(pl.multiple_of(step * blk, blk), blk)

    @pl.when(step == main_steps)
    def _():
        over_out[...] = sums(n_main, n_over)

    @pl.when((step > main_steps) & ((step - main_steps - 1) < extra_ref[0]))
    def _():
        more_out[...] = sums(pl.multiple_of(n_main + OVER_SLOTS + (step - main_steps - 1) * more_blk, more_blk), more_blk)


def grad_rows(extra, ids, slots, c_b, a, e, w_proj, table, n_main, n_over, after=(), tile=512, main_steps=2, more_blk=LANE):
    n_tok, dim = c_b.shape
    n_slot = slots.shape[1]
    n_more = n_slot - n_main - OVER_SLOTS
    want_da = e is not None
    whole = pl.BlockSpec((n_tok, dim), lambda s, *_: (0, 0))
    in_specs = [
        pl.BlockSpec((1, 1, n_tok), lambda s, *_: (table, 0, 0)),
        pl.BlockSpec((1, n_slot, 1), lambda s, *_: (table, 0, 0)),
        whole, whole,
        pl.BlockSpec((1, dim, dim), lambda s, *_: (table, 0, 0)),
    ]

    def more_at(s, extra_ref):
        return (jnp.clip(s - main_steps - 1, 0, jnp.maximum(extra_ref[0] - 1, 0)), 0)

    out_specs = [
        pl.BlockSpec((n_main // main_steps, dim), lambda s, *_: (jnp.minimum(s, main_steps - 1), 0)),
        pl.BlockSpec((n_over, dim), lambda s, *_: (0, 0)),
        pl.BlockSpec((more_blk, dim), more_at),
    ]
    out_shape = [jax.ShapeDtypeStruct((n, dim), F32) for n in (n_main, n_over, n_more)]
    args = [extra, ids, slots, c_b, a, w_proj, *after]
    in_specs += [pl.BlockSpec(memory_space=pl.ANY)] * len(after)
    if want_da:
        in_specs.append(whole)
        out_specs.append(whole)
        out_shape.append(jax.ShapeDtypeStruct((n_tok, dim), BF16))
        args.append(e)
    return pl.pallas_call(
        functools.partial(grad_body, (main_steps, more_blk), tile, want_da, len(after)),
        grid_spec=pltpu.PrefetchScalarGridSpec(
            num_scalar_prefetch=1, grid=(main_steps + 1 + n_more // more_blk,), in_specs=in_specs, out_specs=out_specs,
            scratch_shapes=[pltpu.VMEM((n_tok, dim), BF16)] * 3,
        ),
        out_shape=out_shape,
        compiler_params=params(60, ("arbitrary",)),
        cost_estimate=cost(2 * n_tok * dim * (dim + 3 * 1408), 12 * n_tok * dim),
        name=f"grad_{table}",
    )(*args)


def local_row(key, base, rows_dev):
    row = key - base
    return jnp.where((row >= 0) & (row < rows_dev), row, rows_dev)


def unflatten(flat_sc, tab_ref, rows_dev, parts):
    @pl.loop(0, rows_dev // UNIT)
    def _(i):
        block = tab_ref[0, pl.ds(pl.multiple_of(i * UNIT, UNIT), UNIT), :].astype(F32)
        for p in range(parts):
            flat_sc[pl.ds(i * (UNIT * parts) + p, UNIT, stride=parts), :] = block[:, p * LANE:(p + 1) * LANE]


def pick_unit(slots_ref, src, at, base, rows_dev, parts, flat_sc, stage_sc, out_ref, to):
    for k in range(UNIT):
        row = local_row(slots_ref[src, at + k], base, rows_dev)
        stage_sc[k * parts:(k + 1) * parts, :] = flat_sc[pl.ds(row * parts, parts), :]
    rows = pl.ds(pl.multiple_of(to, UNIT), UNIT)
    for p in range(parts):
        out_ref[rows, p * LANE:(p + 1) * LANE] = stage_sc[pl.ds(p, UNIT, stride=parts), :].astype(BF16)


def serve_body(n_dev, rows_dev, parts, spans, meta_ref, slots_ref, tab_ref, after_ref, *rest):
    del after_ref
    outs, (flat_sc, stage_sc) = rest[:len(spans)], rest[len(spans):]
    me = meta_ref[0]
    base = me * rows_dev
    unflatten(flat_sc, tab_ref, rows_dev, parts)
    flat_sc[rows_dev * parts:(rows_dev + 1) * parts, :] = jnp.zeros((parts, LANE), F32)
    for out_ref, (first, size, skip) in zip(outs, spans):
        direct = skip is None
        if not direct:
            @pl.loop(0, n_dev * size, step=UNIT)
            def _(i):
                out_ref[pl.ds(pl.multiple_of(i, UNIT), UNIT), :] = jnp.zeros((UNIT, parts * LANE), BF16)

        for src in range(n_dev):
            if direct:
                begin, end, at = 0, size // UNIT, first + me * size
            else:
                begin = jnp.clip((meta_ref[1 + src] - skip) // UNIT, 0, size // UNIT)
                end = jnp.clip((meta_ref[1 + n_dev + src] - skip + (UNIT - 1)) // UNIT, 0, size // UNIT)
                at = first

            @pl.loop(begin, end)
            def _(i):
                pick_unit(slots_ref, src, at + i * UNIT, base, rows_dev, parts, flat_sc, stage_sc, out_ref, src * size + i * UNIT)


def serve_rows(meta, slots_all, tables, table, n_dev, spans, after):
    _, rows_dev, dim = tables.shape
    parts = dim // LANE
    sizes = [n_dev * size for _, size, _ in spans]
    return pl.pallas_call(
        functools.partial(serve_body, n_dev, rows_dev, parts, spans),
        grid_spec=pltpu.PrefetchScalarGridSpec(
            num_scalar_prefetch=2, grid=(1,),
            in_specs=[pl.BlockSpec((1, rows_dev, dim), lambda i, *_: (table, 0, 0), pipeline_mode=pl.Buffered(1)), pl.BlockSpec(memory_space=pl.ANY)],
            out_specs=[pl.BlockSpec((n, dim), lambda i, *_: (0, 0), pipeline_mode=pl.Buffered(1)) for n in sizes],
            scratch_shapes=[pltpu.VMEM(((rows_dev + 8) * parts, LANE), F32), pltpu.VMEM((UNIT * parts, LANE), F32)],
        ),
        out_shape=[jax.ShapeDtypeStruct((n, dim), BF16) for n in sizes],
        compiler_params=params(62, ("arbitrary",)),
        cost_estimate=cost(20e9, 22e6),
        name=f"serve_{table}",
    )(meta, slots_all, tables, after)


def collect_body(n_dev, rows_dev, parts, sizes, has_prev, meta_ref, slots_ref, main_ref, over_ref, more_ref, *rest):
    if has_prev:
        rest = rest[1:]
    out_ref, flat_sc, main_sc, over_sc, unit_sc, stage_sc, sems = rest
    step = pl.program_id(0)
    me = meta_ref[0]
    base = me * rows_dev
    n_main, n_over, n_more = sizes

    def part_copy(src, dst, i, n, sem):
        rows = pl.ds(i * n, n)
        return pltpu.make_async_copy(src.at[rows, :], dst.at[rows, :], sem)

    def add_unit(src, at, buf, rows):
        for p in range(parts):
            stage_sc[pl.ds(p, UNIT, stride=parts), :] = buf[rows, p * LANE:(p + 1) * LANE]
        where = [pl.ds(local_row(slots_ref[src, at + k], base, rows_dev) * parts, parts) for k in range(UNIT)]
        sums = [flat_sc[where[k], :] + stage_sc[k * parts:(k + 1) * parts, :] for k in range(UNIT)]
        for k in range(UNIT):
            flat_sc[where[k], :] = sums[k]

    def units(src, first, size):
        begin = jnp.clip((meta_ref[1 + src] - first) // UNIT, 0, size // UNIT)
        end = jnp.clip((meta_ref[1 + n_dev + src] - first + (UNIT - 1)) // UNIT, 0, size // UNIT)
        return begin, end

    @pl.when(step == 0)
    def _():
        for s in range(n_dev):
            part_copy(main_ref, main_sc, s, n_main, sems.at[s]).start()
            part_copy(over_ref, over_sc, s, n_over, sems.at[n_dev + s]).start()

        @pl.loop(0, rows_dev // 8)
        def _(i):
            flat_sc[pl.ds(pl.multiple_of(i * 8 * parts, 8), 8 * parts), :] = jnp.zeros((8 * parts, LANE), F32)

        for s in range(n_dev):
            part_copy(main_ref, main_sc, s, n_main, sems.at[s]).wait()

            @pl.loop(0, (meta_ref[1 + 2 * n_dev + s] + (UNIT - 1)) // UNIT)
            def _(i):
                add_unit(s, me * n_main + i * UNIT, main_sc, pl.ds(pl.multiple_of(s * n_main + i * UNIT, UNIT), UNIT))

        for s in range(n_dev):
            part_copy(over_ref, over_sc, s, n_over, sems.at[n_dev + s]).wait()

            @pl.loop(*units(s, 0, n_over))
            def _(i):
                add_unit(s, n_dev * n_main + i * UNIT, over_sc, pl.ds(pl.multiple_of(s * n_over + i * UNIT, UNIT), UNIT))

        for s in range(n_dev):
            @pl.loop(*units(s, n_over, n_more))
            def _(i):
                rows = pl.ds(pl.multiple_of(s * n_more + i * UNIT, UNIT), UNIT)
                copy = pltpu.make_async_copy(more_ref.at[rows, :], unit_sc, sems.at[2 * n_dev])
                copy.start()
                copy.wait()
                add_unit(s, n_dev * n_main + OVER_SLOTS + i * UNIT, unit_sc, pl.ds(0, UNIT))

    @pl.when(step > 0)
    def _():
        blk = out_ref.shape[1]
        first = (step - 1) * (blk * parts)

        @pl.loop(0, blk // 8)
        def _(i):
            to = pl.ds(pl.multiple_of(i * 8, 8), 8)
            for p in range(parts):
                out_ref[0, to, p * LANE:(p + 1) * LANE] = flat_sc[pl.ds(first + i * (8 * parts) + p, 8, stride=parts), :]


def collect_rows(meta, slots_all, main, over, more, prev, table, n_tables, rows_dev, n_dev, n_blk=6):
    dim = main.shape[1]
    parts = dim // LANE
    blk = rows_dev // n_blk
    any_spec = pl.BlockSpec(memory_space=pl.ANY)
    args = [meta, slots_all, main, over, more]
    alias = {}
    if prev is not None:
        args.append(prev)
        alias = {5: 0}
    return pl.pallas_call(
        functools.partial(collect_body, n_dev, rows_dev, parts, [r.shape[0] // n_dev for r in (main, over, more)], prev is not None),
        grid_spec=pltpu.PrefetchScalarGridSpec(
            num_scalar_prefetch=2, grid=(1 + n_blk,), in_specs=[any_spec] * (len(args) - 2),
            out_specs=pl.BlockSpec((1, blk, dim), lambda i, *_: (table, jnp.maximum(i - 1, 0), 0)),
            scratch_shapes=[
                pltpu.VMEM(((rows_dev + 8) * parts, LANE), F32),
                pltpu.VMEM(main.shape, F32),
                pltpu.VMEM(over.shape, F32),
                pltpu.VMEM((UNIT, dim), F32),
                pltpu.VMEM((UNIT * parts, LANE), F32),
                pltpu.SemaphoreType.DMA((2 * n_dev + 1,)),
            ],
        ),
        out_shape=jax.ShapeDtypeStruct((n_tables, rows_dev, dim), F32),
        input_output_aliases=alias,
        compiler_params=params(56, ("arbitrary",)),
        cost_estimate=cost(20e9, 30e6),
        name=f"collect_{table}",
    )(*args)


def blank(shape, dtype):
    return pl.pallas_call(lambda o: None, out_specs=pl.BlockSpec(memory_space=pl.ANY),
                          out_shape=jax.ShapeDtypeStruct(shape, dtype), name="blank")()


def layout_body(n_dev, cnt_ref, uniq_ref, out_ref):
    n_tab, _, n = uniq_ref.shape
    n_main = n_dev * MAIN
    lane = lax.broadcasted_iota(jnp.int32, (1, n), 1)
    small = lax.broadcasted_iota(jnp.int32, (1, MAIN), 1)
    for j in range(n_tab):
        uniq = uniq_ref[j]
        over = jnp.full((1, n), -1, jnp.int32)
        tail = jnp.zeros((1, LANE), jnp.int32)
        start = jnp.int32(0)
        at = jnp.int32(0)
        for o in range(n_dev):
            cnt = cnt_ref[j, o]
            head = pltpu.roll(uniq, lax.rem(n - start, n), 1)[:, :MAIN]
            out_ref[j, :, o * MAIN:(o + 1) * MAIN] = jnp.where(small < cnt, head, -1)
            extra = jnp.maximum(cnt - MAIN, 0)
            moved = pltpu.roll(uniq, lax.rem(2 * n + at - start - MAIN, n), 1)
            over = jnp.where((lane >= at) & (lane < at + extra), moved, over)
            tail = jnp.where(lax.broadcasted_iota(jnp.int32, (1, LANE), 1) == o, cnt, tail)
            start = start + cnt
            at = at + extra
        left = out_ref.shape[2] - n_main - OVER_SLOTS - LANE
        later = jnp.where(lane < n - OVER, pltpu.roll(over, n - OVER, 1), -1)
        out_ref[j, :, n_main:n_main + OVER_SLOTS] = jnp.where(lane < OVER, over, -1)[:, :OVER_SLOTS]
        out_ref[j, :, n_main + OVER_SLOTS:n_main + OVER_SLOTS + left] = later[:, :left]
        out_ref[j, :, n_main + OVER_SLOTS + left:] = tail


def more_slots(n_tok):
    return -(-(n_tok - OVER) // LANE) * LANE


def route(ids, rows_dev, n_dev):
    n_tab, n_tok = ids.shape
    ordered = lax.sort(ids, dimension=1)
    first = jnp.concatenate([jnp.ones((n_tab, 1), bool), ordered[:, 1:] != ordered[:, :-1]], axis=1)
    lo = (jnp.arange(n_dev, dtype=jnp.int32) * rows_dev)[None, :, None]
    mine = first[:, None, :] & (ordered[:, None, :] >= lo) & (ordered[:, None, :] < lo + rows_dev)
    counts = jnp.sum(mine.astype(jnp.int32), axis=2)
    n_all = n_dev * MAIN + OVER_SLOTS + more_slots(n_tok) + LANE
    uniq = lax.sort(jnp.where(first, ordered, jnp.int32(2 ** 30)), dimension=1)
    return pl.pallas_call(
        functools.partial(layout_body, n_dev),
        grid_spec=pltpu.PrefetchScalarGridSpec(
            num_scalar_prefetch=1, grid=(1,),
            in_specs=[pl.BlockSpec((n_tab, 1, n_tok), lambda i, *_: (0, 0, 0))],
            out_specs=pl.BlockSpec((n_tab, 1, n_all), lambda i, *_: (0, 0, 0))),
        out_shape=jax.ShapeDtypeStruct((n_tab, 1, n_all), jnp.int32),
        name="layout",
    )(counts, uniq.reshape(n_tab, 1, n_tok))


def solution(mesh):
    n_dev = mesh.shape['emb']
    tok_spec = P('emb', None)
    tab_spec = P(None, 'emb', None)

    def local_program(x_start, d_out, token_ids, w_up, w_down, w_gate, w_proj, tables):
        n_tab, n_tok = token_ids.shape[:2]
        rows_dev, dim = tables.shape[1:]
        layers = w_up.shape[0]
        me = lax.axis_index('emb').astype(jnp.int32)
        ids = token_ids.reshape(n_tab, n_tok)
        sent = route(ids, rows_dev, n_dev)
        n_main, n_over, n_more = n_dev * MAIN, OVER, more_slots(n_tok)
        n_slot = n_main + OVER_SLOTS + n_more
        got = lax.all_gather(sent[:, 0], 'emb')
        counts = got[:, :, n_slot:n_slot + n_dev]
        extra = jnp.maximum(counts - MAIN, 0)
        starts = jnp.cumsum(extra, axis=2) - extra
        rest = jnp.sum(extra, axis=2)
        ids_col, ids_row = token_ids, ids.reshape(n_tab, 1, n_tok)
        slots_row = sent[:, :, :n_slot]
        slots_col = slots_row.reshape(n_tab, n_slot, 1)
        plan = []
        for j in range(n_tab):
            to_me = lambda a: lax.dynamic_index_in_dim(a[:, j], me, axis=1, keepdims=False)
            begin = to_me(starts)
            meta = jnp.concatenate([me[None], begin, begin + to_me(extra), jnp.minimum(to_me(counts), MAIN)])
            mine = lax.dynamic_index_in_dim(rest[:, j], me, axis=0, keepdims=True)
            more = jnp.maximum(mine - OVER + (LANE - 1), 0) // LANE
            plan.append(dict(meta=meta, slots=got[:, j, :n_slot], more=more, spill=jnp.any(rest[:, j] > OVER)))

        def fetch(j, after):
            p = plan[j]
            main, over = serve_rows(p['meta'], p['slots'], tables, j, n_dev, ((0, MAIN, None), (n_main, OVER, 0)), after)
            main = lax.all_to_all(main, 'emb', 0, 0, tiled=True)
            over = lax.psum_scatter(over, 'emb', scatter_dimension=0, tiled=True)

            def all_rows():
                (more,) = serve_rows(p['meta'], p['slots'], tables, j, n_dev, ((n_main + OVER_SLOTS, n_more, OVER),), after)
                return lax.psum_scatter(more, 'emb', scatter_dimension=0, tiled=True)

            more = lax.cond(p['spill'], all_rows, lambda: blank((n_more, dim), BF16))
            return main, over, more

        def give_back(j, main, over, more):
            main = lax.all_to_all(main, 'emb', 0, 0, tiled=True)
            over = lax.all_gather(over, 'emb', axis=0, tiled=True)
            more = lax.cond(plan[j]['spill'], lambda: lax.all_gather(more, 'emb', axis=0, tiled=True),
                            lambda: blank((n_dev * n_more, dim), F32))
            return main, over, more

        def collect(j, received, prev):
            return collect_rows(plan[j]['meta'], plan[j]['slots'], *received, prev, j, n_tab, rows_dev, n_dev)

        rows_0 = fetch(0, d_out)
        x_a, m_a, a_0 = fwd_layers(x_start, w_up, w_down, w_gate, 0, 2, 0, False)
        x_2 = mix_rows(plan[0]['more'], ids_col, slots_row, *rows_0, (x_a, m_a, a_0), w_proj, 0)
        rows_1 = fetch(1, x_2)
        x_b, h_b, a_1 = fwd_layers(x_2, w_up, w_down, w_gate, 2, layers - 2, 1, True)
        e_1 = mix_rows(plan[1]['more'], ids_col, slots_row, *rows_1, None, w_proj, 1)
        *sums_1, d_a = grad_rows(plan[1]['more'], ids_row, slots_col, d_out, a_1, e_1, w_proj, 1, n_main, n_over)
        recv_1 = give_back(1, *sums_1)
        c_b = bwd_layers(d_out, x_b, h_b, w_up, w_down, d_a, w_gate, layers - 1, 1)
        sums_0 = grad_rows(plan[0]['more'], ids_row, slots_col, c_b, a_0, None, w_proj, 0, n_main, n_over, after=recv_1[:2])
        recv_0 = give_back(0, *sums_0)
        x_end = finish(sums_0[1], x_b, h_b, a_1, e_1, w_down, w_proj, layers - 1, 1)
        grads = collect(0, recv_0, collect(1, recv_1, None))
        return x_end, grads

    return jax.shard_map(local_program, mesh=mesh, in_specs=(tok_spec, tok_spec, tab_spec, P(), P(), P(), P(), tab_spec), out_specs=(tok_spec, tab_spec), check_vma=False)
```

```python
import functools

import jax
import jax.numpy as jnp
from jax import lax
from jax.experimental import pallas as pl
from jax.experimental.pallas import tpu as pltpu
from jax.sharding import PartitionSpec as P

EPS = 1e-6
GELU_K = 0.7978845608028654
GELU_C = 0.044715
F32 = jnp.float32
BF16 = jnp.bfloat16
UNIT = 16
LANE = 128
SUB = 256
MAIN = 128
OVER = 320
OVER_SLOTS = 384
NT = (((1,), (1,)), ((), ()))
NN = (((1,), (0,)), ((), ()))


def dot(a, b, dims=NN):
    return lax.dot_general(a, b, dims, preferred_element_type=F32)


def gelu(v):
    half = 0.5 * v
    return half + half * jnp.tanh(v * (GELU_K + (GELU_K * GELU_C) * (v * v)))


def gelu_grad(v):
    sq = v * v
    th = jnp.tanh(v * (GELU_K + (GELU_K * GELU_C) * sq))
    return (0.5 + 0.5 * th) * (1.0 + (v * (GELU_K + (3.0 * GELU_K * GELU_C) * sq)) * (1.0 - th))


def params(mb, sem=None):
    return pltpu.CompilerParams(vmem_limit_bytes=mb * 1024 * 1024, dimension_semantics=sem)


def cost(flops, nbytes):
    return pl.CostEstimate(flops=int(flops), bytes_accessed=int(nbytes), transcendentals=0)


def fwd_body(n_lay, tile, chunk, save_h, plain, x0_ref, up_ref, dn_ref, gate_ref, after_ref, *rest):
    del after_ref
    if save_h:
        x_out, h_out, a_out, x_sc = rest
    elif plain:
        m_out, x_sc = rest
    else:
        x_out, m_out, a_out, x_sc = rest
    lay, blk = pl.program_id(0), pl.program_id(1)
    rows = pl.ds(pl.multiple_of(blk * tile, tile), tile)

    @pl.when(lay == 0)
    def _():
        x_sc[rows, :] = x0_ref[...]

    x_bf = x_sc[rows, :]
    if not plain:
        x_out[0] = x_bf
    x_f = x_bf.astype(F32)
    inv = lax.rsqrt(jnp.mean(x_f * x_f, axis=-1, keepdims=True) + EPS)
    u = (x_f * inv).astype(BF16)
    sub = min(tile, SUB)
    ff = up_ref.shape[2]
    todo = [(r, lo) for r in range(0, tile, sub) for lo in range(0, ff, chunk)]
    up_dot = lambda r, lo: dot(u[r:r + sub, :], up_ref[0, :, lo:lo + chunk])

    def mlp():
        nxt = up_dot(*todo[0])
        accs = {}
        for i, (r, lo) in enumerate(todo):
            h = nxt.astype(BF16)
            if i + 1 < len(todo):
                nxt = up_dot(*todo[i + 1])
            if save_h:
                h_out[0, r:r + sub, lo:lo + chunk] = h
            act = gelu(h.astype(F32)).astype(BF16)
            part = dot(act, dn_ref[0, lo:lo + chunk, :])
            accs[r] = part if lo == 0 else accs[r] + part
        return jnp.concatenate([accs[r].astype(BF16) for r in sorted(accs)], axis=0)

    if save_h:
        @pl.when(lay < n_lay - 1)
        def _():
            x_sc[rows, :] = (x_f + mlp().astype(F32)).astype(BF16)

        @pl.when(lay == n_lay - 1)
        def _():
            h_out[0] = dot(u, up_ref[0]).astype(BF16)
    elif plain:
        m_out[...] = (x_f + mlp().astype(F32)).astype(BF16)
        return
    else:
        m = mlp()
        x_sc[rows, :] = (x_f + m.astype(F32)).astype(BF16)

    @pl.when(lay == n_lay - 1)
    def _():
        if not save_h:
            m_out[...] = m
        a_out[...] = dot(u, gate_ref[0]).astype(BF16)


def fwd_layers(x0, w_up, w_down, w_gate, first, n_lay, table, save_h, after, plain=False, tile=512, chunk=3072):
    n_tok, dim = x0.shape
    ff = w_up.shape[2]
    last = n_lay - 1
    in_specs = [
        pl.BlockSpec((tile, dim), lambda l, t: (jnp.where(l == 0, t, n_tok // tile - 1), 0)),
        pl.BlockSpec((1, dim, ff), lambda l, t: (first + l, 0, 0)),
        pl.BlockSpec((1, ff, dim), lambda l, t: (first + l, 0, 0)),
        pl.BlockSpec((1, dim, dim), lambda l, t: (table, 0, 0)),
        pl.BlockSpec(memory_space=pl.ANY),
    ]
    end = pl.BlockSpec((tile, dim), lambda l, t: (jnp.where(l == last, t, 0), 0))
    out_specs = [pl.BlockSpec((1, tile, dim), lambda l, t: (l, t, 0))]
    out_shape = [jax.ShapeDtypeStruct((n_lay, n_tok, dim), BF16)]
    if save_h:
        out_specs.append(pl.BlockSpec((1, tile, ff), lambda l, t: (l, t, 0)))
        out_shape.append(jax.ShapeDtypeStruct((n_lay, n_tok, ff), BF16))
    if plain:
        out_specs, out_shape = [], []
    n_end = 1 if save_h or plain else 2
    out_specs += [end] * n_end
    out_shape += [jax.ShapeDtypeStruct((n_tok, dim), BF16)] * n_end
    return pl.pallas_call(
        functools.partial(fwd_body, n_lay, tile, chunk, save_h, plain),
        grid=(n_lay, n_tok // tile), in_specs=in_specs, out_specs=out_specs, out_shape=out_shape,
        scratch_shapes=[pltpu.VMEM((n_tok, dim), BF16)],
        compiler_params=params(60, ("arbitrary", "arbitrary")),
        cost_estimate=cost(n_lay * 4 * n_tok * dim * ff, n_lay * (4 * dim * ff + 2 * n_tok * ff)),
        name=f"fwd_{first}",
    )(x0, w_up, w_down, w_gate, after)


def bwd_body(n_lay, tile, chunk, c0_ref, x_ref, h_ref, up_ref, dn_ref, da_ref, gate_ref, cb_out, c_sc, du_sc):
    step, blk = pl.program_id(0), pl.program_id(1)
    rows = pl.ds(pl.multiple_of(blk * tile, tile), tile)

    @pl.when(step == 0)
    def _():
        c_sc[rows, :] = c0_ref[...].astype(F32)

    c_b = c_sc[rows, :].astype(BF16)
    sub = tile
    ff = up_ref.shape[2]
    todo = [(r, lo) for r in range(0, tile, sub) for lo in range(0, ff, chunk)]
    act_dot = lambda r, lo: dot(c_b[r:r + sub, :], dn_ref[0, lo:lo + chunk, :], NT)
    nxt = act_dot(*todo[0])
    for i, (r, lo) in enumerate(todo):
        d_act = nxt
        if i + 1 < len(todo):
            nxt = act_dot(*todo[i + 1])
        d_h = (gelu_grad(h_ref[0, r:r + sub, lo:lo + chunk].astype(F32)) * d_act).astype(BF16)
        part = dot(d_h, up_ref[0, :, lo:lo + chunk], NT)
        if lo == 0:
            du_sc[r:r + sub, :] = part
        else:
            du_sc[r:r + sub, :] += part

    @pl.when(step == 0)
    def _():
        du_sc[...] += dot(da_ref[...], gate_ref[0], NT)

    x_f = x_ref[0].astype(F32)
    inv = lax.rsqrt(jnp.mean(x_f * x_f, axis=-1, keepdims=True) + EPS)
    du = du_sc[...]
    c_new = c_sc[rows, :] + (inv * du - x_f * (inv * inv * inv) * jnp.mean(x_f * du, axis=-1, keepdims=True))
    c_sc[rows, :] = c_new

    @pl.when(step == n_lay - 1)
    def _():
        cb_out[...] = c_new.astype(BF16)


def bwd_layers(c0, x_all, h_all, w_up, w_down, d_gate, w_gate, last_layer, table, tile=512, chunk=1536):
    n_lay, n_tok, dim = x_all.shape
    ff = w_up.shape[2]
    end_blk = n_tok // tile - 1
    first_only = pl.BlockSpec((tile, dim), lambda i, t: (jnp.where(i == 0, t, end_blk), 0))
    return pl.pallas_call(
        functools.partial(bwd_body, n_lay, tile, chunk),
        grid=(n_lay, n_tok // tile),
        in_specs=[
            first_only,
            pl.BlockSpec((1, tile, dim), lambda i, t: (n_lay - 1 - i, t, 0)),
            pl.BlockSpec((1, tile, ff), lambda i, t: (n_lay - 1 - i, t, 0)),
            pl.BlockSpec((1, dim, ff), lambda i, t: (last_layer - i, 0, 0)),
            pl.BlockSpec((1, ff, dim), lambda i, t: (last_layer - i, 0, 0)),
            first_only,
            pl.BlockSpec((1, dim, dim), lambda i, t: (table, 0, 0)),
        ],
        out_specs=pl.BlockSpec((tile, dim), lambda i, t: (jnp.where(i == n_lay - 1, t, 0), 0)),
        out_shape=jax.ShapeDtypeStruct((n_tok, dim), BF16),
        scratch_shapes=[pltpu.VMEM((n_tok, dim), F32), pltpu.VMEM((tile, dim), F32)],
        compiler_params=params(60, ("arbitrary", "arbitrary")),
        cost_estimate=cost(n_lay * 4 * n_tok * dim * ff, n_lay * (4 * dim * ff + 2 * n_tok * ff)),
        name="bwd",
    )(c0, x_all, h_all, w_up, w_down, d_gate, w_gate)


def expand(n_main, n_over, blk, extra_ref, ids_ref, slots_ref, main_ref, over_ref, more_ref, acc):
    keys = ids_ref[0]
    lo = n_main + OVER_SLOTS
    acc[...] = (dot((keys == slots_ref[0, :, :n_main]).astype(BF16), main_ref[...])
                + dot((keys == slots_ref[0, :, n_main:n_main + n_over]).astype(BF16), over_ref[...]))

    @pl.loop(0, extra_ref[0])
    def _(i):
        at = pl.multiple_of(i * blk, blk)
        hit = (keys == slots_ref[0, :, pl.ds(lo + at, blk)]).astype(BF16)
        acc[...] += dot(hit, more_ref[pl.ds(at, blk), :])

    return acc[...]


def gated(a_ref, e_f, proj_ref):
    g = gelu(a_ref[...].astype(F32)).astype(BF16).astype(F32)
    return dot((g * e_f).astype(BF16), proj_ref[0]).astype(BF16).astype(F32)


def mix_body(n_main, n_over, blk, extra_ref, ids_ref, slots_ref, main_ref, over_ref, more_ref, x_ref, m_ref, a_ref, proj_ref, x_out, acc):
    e_f = expand(n_main, n_over, blk, extra_ref, ids_ref, slots_ref, main_ref, over_ref, more_ref, acc)
    q = gated(a_ref, e_f, proj_ref)
    x_out[...] = ((x_ref[0].astype(F32) + m_ref[...].astype(F32)) + q).astype(BF16)


def expand_body(n_main, n_over, blk, extra_ref, ids_ref, slots_ref, main_ref, over_ref, more_ref, e_out, acc):
    e_out[...] = expand(n_main, n_over, blk, extra_ref, ids_ref, slots_ref, main_ref, over_ref, more_ref, acc).astype(BF16)


def mix_rows(extra, ids, slots, main, over, more, layer_args, w_proj, table, tile=512, blk=LANE):
    n_tok, dim = ids.shape[1], main.shape[1]
    n_slot = slots.shape[2]
    tok = pl.BlockSpec((tile, dim), lambda t, *_: (t, 0))
    whole = lambda arr: pl.BlockSpec(arr.shape, lambda t, *_: (0, 0))
    in_specs = [
        pl.BlockSpec((1, tile, 1), lambda t, *_: (table, t, 0)),
        pl.BlockSpec((1, 1, n_slot), lambda t, *_: (table, 0, 0)),
        whole(main), whole(over), whole(more),
    ]
    args = [extra, ids, slots, main, over, more]
    if layer_args is not None:
        last = layer_args[0].shape[0] - 1
        in_specs += [
            pl.BlockSpec((1, tile, dim), lambda t, *_: (last, t, 0)), tok, tok,
            pl.BlockSpec((1, dim, dim), lambda t, *_: (table, 0, 0)),
        ]
        args += [*layer_args, w_proj]
    return pl.pallas_call(
        functools.partial(expand_body if layer_args is None else mix_body, main.shape[0], over.shape[0], blk),
        grid_spec=pltpu.PrefetchScalarGridSpec(
            num_scalar_prefetch=1, grid=(n_tok // tile,), in_specs=in_specs, out_specs=tok,
            scratch_shapes=[pltpu.VMEM((tile, dim), F32)],
        ),
        out_shape=jax.ShapeDtypeStruct((n_tok, dim), BF16),
        compiler_params=params(48, ("arbitrary",)),
        cost_estimate=cost(2 * n_tok * dim * (dim + 1344), 12 * n_tok * dim),
        name=f"mix_{table}",
    )(*args)


def finish_body(chunk, after_ref, x_ref, h_ref, a_ref, e_ref, dn_ref, proj_ref, x_out):
    del after_ref
    q = gated(a_ref, e_ref[...].astype(F32), proj_ref)
    acc = None
    for lo in range(0, h_ref.shape[2], chunk):
        act = gelu(h_ref[0, :, lo:lo + chunk].astype(F32)).astype(BF16)
        part = dot(act, dn_ref[0, lo:lo + chunk, :])
        acc = part if acc is None else acc + part
    x_out[...] = ((x_ref[0].astype(F32) + acc.astype(BF16).astype(F32)) + q).astype(BF16)


def finish(after, x_all, h_all, a, e, w_down, w_proj, layer, table, tile=512, chunk=1024):
    n_lay, n_tok, dim = x_all.shape
    ff = h_all.shape[2]
    tok = pl.BlockSpec((tile, dim), lambda t: (t, 0))
    return pl.pallas_call(
        functools.partial(finish_body, chunk),
        grid=(n_tok // tile,),
        in_specs=[
            pl.BlockSpec(memory_space=pl.ANY),
            pl.BlockSpec((1, tile, dim), lambda t: (n_lay - 1, t, 0)),
            pl.BlockSpec((1, tile, ff), lambda t: (n_lay - 1, t, 0)),
            tok, tok,
            pl.BlockSpec((1, ff, dim), lambda t: (layer, 0, 0)),
            pl.BlockSpec((1, dim, dim), lambda t: (table, 0, 0)),
        ],
        out_specs=tok,
        out_shape=jax.ShapeDtypeStruct((n_tok, dim), BF16),
        compiler_params=params(48, ("arbitrary",)),
        cost_estimate=cost(2 * n_tok * dim * (dim + ff), 6 * n_tok * dim + 2 * n_tok * ff),
        name="finish",
    )(after, x_all, h_all, a, e, w_down, w_proj)


def grad_body(steps, tile, want_da, kind, n_after, extra_ref, ids_ref, slots_ref, c_ref, a_ref, proj_ref, *rest):
    rest = rest[n_after:]
    rest, (hi_sc, mid_sc, lo_sc) = list(rest[:-3]), rest[-3:]
    e_ref = rest.pop(0) if want_da else None
    main_out = rest.pop(0) if kind != "over" else None
    over_out, more_out = (rest.pop(0), rest.pop(0)) if kind != "main" else (None, None)
    da_out = rest.pop(0) if want_da else None
    step = pl.program_id(0)
    main_steps, more_blk, n_main = steps

    @pl.when(step == 0)
    def _():
        @pl.loop(0, c_ref.shape[0], step=tile)
        def _(lo):
            rows = pl.ds(pl.multiple_of(lo, tile), tile)
            dz = dot(c_ref[rows, :], proj_ref[0], NT)
            a_f = a_ref[rows, :].astype(F32)
            g = gelu(a_f).astype(BF16).astype(F32)
            if want_da:
                da_out[rows, :] = (gelu_grad(a_f) * (dz * e_ref[rows, :].astype(F32))).astype(BF16)
            grad = g * dz
            hi = grad.astype(BF16)
            left = grad - hi.astype(F32)
            mid = left.astype(BF16)
            hi_sc[rows, :] = hi
            mid_sc[rows, :] = mid
            lo_sc[rows, :] = (left - mid.astype(F32)).astype(BF16)

    def sums(first, size):
        hit = (slots_ref[0, pl.ds(first, size), :] == ids_ref[0]).astype(BF16)
        return (dot(hit, lo_sc[...]) + dot(hit, mid_sc[...])) + dot(hit, hi_sc[...])

    if kind != "over":
        @pl.when(step < main_steps)
        def _():
            blk = main_out.shape[0]
            main_out[...] = sums(pl.multiple_of(step * blk, blk), blk)

    if kind != "main":
        @pl.when(step == main_steps)
        def _():
            over_out[...] = sums(n_main, over_out.shape[0])

        @pl.when((step > main_steps) & ((step - main_steps - 1) < extra_ref[0]))
        def _():
            more_out[...] = sums(pl.multiple_of(n_main + OVER_SLOTS + (step - main_steps - 1) * more_blk, more_blk), more_blk)


def grad_rows(extra, ids, slots, c_b, a, e, w_proj, table, n_main, n_over, after=(), kind="both", tile=512, main_steps=2, more_blk=LANE):
    n_tok, dim = c_b.shape
    n_slot = slots.shape[1]
    n_more = n_slot - n_main - OVER_SLOTS
    main_steps = 0 if kind == "over" else main_steps
    want_da = e is not None
    whole = pl.BlockSpec((n_tok, dim), lambda s, *_: (0, 0))
    in_specs = [
        pl.BlockSpec((1, 1, n_tok), lambda s, *_: (table, 0, 0)),
        pl.BlockSpec((1, n_slot, 1), lambda s, *_: (table, 0, 0)),
        whole, whole,
        pl.BlockSpec((1, dim, dim), lambda s, *_: (table, 0, 0)),
    ]

    def more_at(s, extra_ref):
        return (jnp.clip(s - main_steps - 1, 0, jnp.maximum(extra_ref[0] - 1, 0)), 0)

    out_specs, out_shape = [], []
    if kind != "over":
        out_specs.append(pl.BlockSpec((n_main // main_steps, dim), lambda s, *_: (jnp.minimum(s, main_steps - 1), 0)))
        out_shape.append(jax.ShapeDtypeStruct((n_main, dim), F32))
    if kind != "main":
        out_specs += [pl.BlockSpec((n_over, dim), lambda s, *_: (0, 0)), pl.BlockSpec((more_blk, dim), more_at)]
        out_shape += [jax.ShapeDtypeStruct((n, dim), F32) for n in (n_over, n_more)]
    n_steps = main_steps if kind == "main" else main_steps + 1 + n_more // more_blk
    args = [extra, ids, slots, c_b, a, w_proj, *after]
    in_specs += [pl.BlockSpec(memory_space=pl.ANY)] * len(after)
    if want_da:
        in_specs.append(whole)
        out_specs.append(whole)
        out_shape.append(jax.ShapeDtypeStruct((n_tok, dim), BF16))
        args.append(e)
    return pl.pallas_call(
        functools.partial(grad_body, (main_steps, more_blk, n_main), tile, want_da, kind, len(after)),
        grid_spec=pltpu.PrefetchScalarGridSpec(
            num_scalar_prefetch=1, grid=(n_steps,), in_specs=in_specs, out_specs=out_specs,
            scratch_shapes=[pltpu.VMEM((n_tok, dim), BF16)] * 3,
        ),
        out_shape=out_shape,
        compiler_params=params(60, ("arbitrary",)),
        cost_estimate=cost(2 * n_tok * dim * (dim + 3 * (n_main if kind == "main" else n_over)), 12 * n_tok * dim),
        name=f"grad_{table}_{kind}",
    )(*args)


def local_row(key, base, rows_dev):
    row = key - base
    return jnp.where((row >= 0) & (row < rows_dev), row, rows_dev)


def unflatten(flat_sc, tab_ref, rows_dev, parts):
    @pl.loop(0, rows_dev // UNIT, unroll=3)
    def _(i):
        block = tab_ref[0, pl.ds(pl.multiple_of(i * UNIT, UNIT), UNIT), :].astype(F32)
        for p in range(parts):
            flat_sc[pl.ds(i * (UNIT * parts) + p, UNIT, stride=parts), :] = block[:, p * LANE:(p + 1) * LANE]


def pick_unit(slots_ref, src, at, base, rows_dev, parts, flat_sc, stage_sc, out_ref, to):
    for k in range(UNIT):
        row = local_row(slots_ref[src, at + k], base, rows_dev)
        stage_sc[k * parts:(k + 1) * parts, :] = flat_sc[pl.ds(row * parts, parts), :]
    rows = pl.ds(pl.multiple_of(to, UNIT), UNIT)
    for p in range(parts):
        out_ref[rows, p * LANE:(p + 1) * LANE] = stage_sc[pl.ds(p, UNIT, stride=parts), :].astype(BF16)


def serve_body(n_dev, rows_dev, parts, spans, meta_ref, slots_ref, tab_ref, after_ref, *rest):
    del after_ref
    outs, (flat_sc, stage_sc) = rest[:len(spans)], rest[len(spans):]
    me = meta_ref[0]
    base = me * rows_dev
    unflatten(flat_sc, tab_ref, rows_dev, parts)
    flat_sc[rows_dev * parts:(rows_dev + 1) * parts, :] = jnp.zeros((parts, LANE), F32)
    for out_ref, (first, size, skip) in zip(outs, spans):
        direct = skip is None
        if not direct:
            @pl.loop(0, n_dev * size, step=UNIT)
            def _(i):
                out_ref[pl.ds(pl.multiple_of(i, UNIT), UNIT), :] = jnp.zeros((UNIT, parts * LANE), BF16)

        for src in range(n_dev):
            if direct:
                begin, end, at = 0, size // UNIT, first + me * size
            else:
                begin = jnp.clip((meta_ref[1 + src] - skip) // UNIT, 0, size // UNIT)
                end = jnp.clip((meta_ref[1 + n_dev + src] - skip + (UNIT - 1)) // UNIT, 0, size // UNIT)
                at = first

            @pl.loop(begin, end)
            def _(i):
                pick_unit(slots_ref, src, at + i * UNIT, base, rows_dev, parts, flat_sc, stage_sc, out_ref, src * size + i * UNIT)


def serve_rows(meta, slots_all, tables, table, n_dev, spans, after):
    _, rows_dev, dim = tables.shape
    parts = dim // LANE
    sizes = [n_dev * size for _, size, _ in spans]
    return pl.pallas_call(
        functools.partial(serve_body, n_dev, rows_dev, parts, spans),
        grid_spec=pltpu.PrefetchScalarGridSpec(
            num_scalar_prefetch=2, grid=(1,),
            in_specs=[pl.BlockSpec((1, rows_dev, dim), lambda i, *_: (table, 0, 0), pipeline_mode=pl.Buffered(1)), pl.BlockSpec(memory_space=pl.ANY)],
            out_specs=[pl.BlockSpec((n, dim), lambda i, *_: (0, 0), pipeline_mode=pl.Buffered(1)) for n in sizes],
            scratch_shapes=[pltpu.VMEM(((rows_dev + 8) * parts, LANE), F32), pltpu.VMEM((UNIT * parts, LANE), F32)],
        ),
        out_shape=[jax.ShapeDtypeStruct((n, dim), BF16) for n in sizes],
        compiler_params=params(62, ("arbitrary",)),
        cost_estimate=cost(1e6, 1e4),
        name=f"serve_{table}",
    )(meta, slots_all, tables, after)


def collect_body(n_dev, rows_dev, parts, sizes, has_prev, meta_ref, slots_ref, main_ref, over_ref, more_ref, *rest):
    if has_prev:
        rest = rest[1:]
    out_ref, flat_sc, main_sc, over_sc, unit_sc, stage_sc, sems = rest
    step = pl.program_id(0)
    me = meta_ref[0]
    base = me * rows_dev
    n_main, n_over, n_more = sizes

    def part_copy(src, dst, i, n, sem):
        rows = pl.ds(i * n, n)
        return pltpu.make_async_copy(src.at[rows, :], dst.at[rows, :], sem)

    def add_unit(src, at, buf, rows):
        for p in range(parts):
            stage_sc[pl.ds(p, UNIT, stride=parts), :] = buf[rows, p * LANE:(p + 1) * LANE]
        where = [pl.ds(local_row(slots_ref[src, at + k], base, rows_dev) * parts, parts) for k in range(UNIT)]
        sums = [flat_sc[where[k], :] + stage_sc[k * parts:(k + 1) * parts, :] for k in range(UNIT)]
        for k in range(UNIT):
            flat_sc[where[k], :] = sums[k]

    def units(src, first, size):
        begin = jnp.clip((meta_ref[1 + src] - first) // UNIT, 0, size // UNIT)
        end = jnp.clip((meta_ref[1 + n_dev + src] - first + (UNIT - 1)) // UNIT, 0, size // UNIT)
        return begin, end

    @pl.when(step == 0)
    def _():
        for s in range(n_dev):
            part_copy(main_ref, main_sc, s, n_main, sems.at[s]).start()
            part_copy(over_ref, over_sc, s, n_over, sems.at[n_dev + s]).start()

        @pl.loop(0, rows_dev // 8, unroll=6)
        def _(i):
            flat_sc[pl.ds(pl.multiple_of(i * 8 * parts, 8), 8 * parts), :] = jnp.zeros((8 * parts, LANE), F32)

        for s in range(n_dev):
            part_copy(main_ref, main_sc, s, n_main, sems.at[s]).wait()

            @pl.loop(0, (meta_ref[1 + 2 * n_dev + s] + (UNIT - 1)) // UNIT)
            def _(i):
                add_unit(s, me * n_main + i * UNIT, main_sc, pl.ds(pl.multiple_of(s * n_main + i * UNIT, UNIT), UNIT))

        for s in range(n_dev):
            part_copy(over_ref, over_sc, s, n_over, sems.at[n_dev + s]).wait()

            @pl.loop(*units(s, 0, n_over))
            def _(i):
                add_unit(s, n_dev * n_main + i * UNIT, over_sc, pl.ds(pl.multiple_of(s * n_over + i * UNIT, UNIT), UNIT))

        for s in range(n_dev):
            @pl.loop(*units(s, n_over, n_more))
            def _(i):
                rows = pl.ds(pl.multiple_of(s * n_more + i * UNIT, UNIT), UNIT)
                copy = pltpu.make_async_copy(more_ref.at[rows, :], unit_sc, sems.at[2 * n_dev])
                copy.start()
                copy.wait()
                add_unit(s, n_dev * n_main + OVER_SLOTS + i * UNIT, unit_sc, pl.ds(0, UNIT))

    @pl.when(step > 0)
    def _():
        blk = out_ref.shape[1]
        first = (step - 1) * (blk * parts)

        def put(i):
            to = pl.ds(pl.multiple_of(i * 8, 8), 8)
            for p in range(parts):
                out_ref[0, to, p * LANE:(p + 1) * LANE] = flat_sc[pl.ds(first + i * (8 * parts) + p, 8, stride=parts), :]

        many = 8

        @pl.loop(0, blk // (8 * many))
        def _(i):
            for k in range(many):
                put(i * many + k)

        for k in range(blk // (8 * many) * many, blk // 8):
            put(k)


def collect_rows(meta, slots_all, main, over, more, prev, table, n_tables, rows_dev, n_dev, n_blk=6):
    dim = main.shape[1]
    parts = dim // LANE
    blk = rows_dev // n_blk
    any_spec = pl.BlockSpec(memory_space=pl.ANY)
    args = [meta, slots_all, main, over, more]
    alias = {}
    if prev is not None:
        args.append(prev)
        alias = {5: 0}
    return pl.pallas_call(
        functools.partial(collect_body, n_dev, rows_dev, parts, [r.shape[0] // n_dev for r in (main, over, more)], prev is not None),
        grid_spec=pltpu.PrefetchScalarGridSpec(
            num_scalar_prefetch=2, grid=(1 + n_blk,), in_specs=[any_spec] * (len(args) - 2),
            out_specs=pl.BlockSpec((1, blk, dim), lambda i, *_: (table, jnp.maximum(i - 1, 0), 0)),
            scratch_shapes=[
                pltpu.VMEM(((rows_dev + 8) * parts, LANE), F32),
                pltpu.VMEM(main.shape, F32),
                pltpu.VMEM(over.shape, F32),
                pltpu.VMEM((UNIT, dim), F32),
                pltpu.VMEM((UNIT * parts, LANE), F32),
                pltpu.SemaphoreType.DMA((2 * n_dev + 1,)),
            ],
        ),
        out_shape=jax.ShapeDtypeStruct((n_tables, rows_dev, dim), F32),
        input_output_aliases=alias,
        compiler_params=params(56, ("arbitrary",)),
        cost_estimate=cost(20e9, 30e6),
        name=f"collect_{table}",
    )(*args)


def blank(shape, dtype):
    return pl.pallas_call(lambda o: None, out_specs=pl.BlockSpec(memory_space=pl.ANY),
                          out_shape=jax.ShapeDtypeStruct(shape, dtype), name="blank")()


def layout_body(n_dev, cnt_ref, uniq_ref, after_ref, out_ref):
    del after_ref
    n_tab, _, n = uniq_ref.shape
    n_main = n_dev * MAIN
    lane = lax.broadcasted_iota(jnp.int32, (1, n), 1)
    small = lax.broadcasted_iota(jnp.int32, (1, MAIN), 1)
    for j in range(n_tab):
        uniq = uniq_ref[j]
        over = jnp.full((1, n), -1, jnp.int32)
        tail = jnp.zeros((1, LANE), jnp.int32)
        start = jnp.int32(0)
        at = jnp.int32(0)
        for o in range(n_dev):
            cnt = cnt_ref[j, o]
            head = pltpu.roll(uniq, lax.rem(n - start, n), 1)[:, :MAIN]
            out_ref[j, :, o * MAIN:(o + 1) * MAIN] = jnp.where(small < cnt, head, -1)
            extra = jnp.maximum(cnt - MAIN, 0)
            moved = pltpu.roll(uniq, lax.rem(2 * n + at - start - MAIN, n), 1)
            over = jnp.where((lane >= at) & (lane < at + extra), moved, over)
            tail = jnp.where(lax.broadcasted_iota(jnp.int32, (1, LANE), 1) == o, cnt, tail)
            start = start + cnt
            at = at + extra
        left = out_ref.shape[2] - n_main - OVER_SLOTS - LANE
        later = jnp.where(lane < n - OVER, pltpu.roll(over, n - OVER, 1), -1)
        out_ref[j, :, n_main:n_main + OVER_SLOTS] = jnp.where(lane < OVER, over, -1)[:, :OVER_SLOTS]
        out_ref[j, :, n_main + OVER_SLOTS:n_main + OVER_SLOTS + left] = later[:, :left]
        out_ref[j, :, n_main + OVER_SLOTS + left:] = tail


def more_slots(n_tok):
    return -(-(n_tok - OVER) // LANE) * LANE


def route(ids, rows_dev, n_dev, after):
    n_tab, n_tok = ids.shape
    ordered = lax.sort(ids, dimension=1)
    first = jnp.concatenate([jnp.ones((n_tab, 1), bool), ordered[:, 1:] != ordered[:, :-1]], axis=1)
    lo = (jnp.arange(n_dev, dtype=jnp.int32) * rows_dev)[None, :, None]
    mine = first[:, None, :] & (ordered[:, None, :] >= lo) & (ordered[:, None, :] < lo + rows_dev)
    counts = jnp.sum(mine.astype(jnp.int32), axis=2)
    n_all = n_dev * MAIN + OVER_SLOTS + more_slots(n_tok) + LANE
    uniq = lax.sort(jnp.where(first, ordered, jnp.int32(2 ** 30)), dimension=1)
    return pl.pallas_call(
        functools.partial(layout_body, n_dev),
        grid_spec=pltpu.PrefetchScalarGridSpec(
            num_scalar_prefetch=1, grid=(1,),
            in_specs=[pl.BlockSpec((n_tab, 1, n_tok), lambda i, *_: (0, 0, 0)), pl.BlockSpec(memory_space=pl.ANY)],
            out_specs=pl.BlockSpec((n_tab, 1, n_all), lambda i, *_: (0, 0, 0))),
        out_shape=jax.ShapeDtypeStruct((n_tab, 1, n_all), jnp.int32),
        name="layout",
    )(counts, uniq.reshape(n_tab, 1, n_tok), after)


def solution(mesh):
    n_dev = mesh.shape['emb']
    tok_spec = P('emb', None)
    tab_spec = P(None, 'emb', None)

    def local_program(x_start, d_out, token_ids, w_up, w_down, w_gate, w_proj, tables):
        n_tab, n_tok = token_ids.shape[:2]
        rows_dev, dim = tables.shape[1:]
        layers = w_up.shape[0]
        me = lax.axis_index('emb').astype(jnp.int32)
        ids = token_ids.reshape(n_tab, n_tok)
        (x_1,) = fwd_layers(x_start, w_up, w_down, w_gate, 0, 1, 0, False, d_out, plain=True)
        sent = route(ids, rows_dev, n_dev, x_1)
        n_main, n_over, n_more = n_dev * MAIN, OVER, more_slots(n_tok)
        n_slot = n_main + OVER_SLOTS + n_more
        got = lax.all_gather(sent[:, 0], 'emb')
        counts = got[:, :, n_slot:n_slot + n_dev]
        extra = jnp.maximum(counts - MAIN, 0)
        starts = jnp.cumsum(extra, axis=2) - extra
        rest = jnp.sum(extra, axis=2)
        ids_col, ids_row = token_ids, ids.reshape(n_tab, 1, n_tok)
        slots_row = sent[:, :, :n_slot]
        slots_col = slots_row.reshape(n_tab, n_slot, 1)
        plan = []
        for j in range(n_tab):
            to_me = lambda a: lax.dynamic_index_in_dim(a[:, j], me, axis=1, keepdims=False)
            begin = to_me(starts)
            meta = jnp.concatenate([me[None], begin, begin + to_me(extra), jnp.minimum(to_me(counts), MAIN)])
            mine = lax.dynamic_index_in_dim(rest[:, j], me, axis=0, keepdims=True)
            more = jnp.maximum(mine - OVER + (LANE - 1), 0) // LANE
            plan.append(dict(meta=meta, slots=got[:, j, :n_slot], more=more, spill=jnp.any(rest[:, j] > OVER)))

        def serve(j, after):
            p = plan[j]
            return serve_rows(p['meta'], p['slots'], tables, j, n_dev, ((0, MAIN, None), (n_main, OVER, 0)), after)

        def fetch(j, main, over, after):
            p = plan[j]
            main = lax.all_to_all(main, 'emb', 0, 0, tiled=True)
            over = lax.psum_scatter(over, 'emb', scatter_dimension=0, tiled=True)

            def all_rows():
                (more,) = serve_rows(p['meta'], p['slots'], tables, j, n_dev, ((n_main + OVER_SLOTS, n_more, OVER),), after)
                return lax.psum_scatter(more, 'emb', scatter_dimension=0, tiled=True)

            more = lax.cond(p['spill'], all_rows, lambda: blank((n_more, dim), BF16))
            return main, over, more

        def give_back(j, main, over, more):
            main = lax.all_to_all(main, 'emb', 0, 0, tiled=True)
            over = lax.all_gather(over, 'emb', axis=0, tiled=True)
            more = lax.cond(plan[j]['spill'], lambda: lax.all_gather(more, 'emb', axis=0, tiled=True),
                            lambda: blank((n_dev * n_more, dim), F32))
            return main, over, more

        def collect(j, received, prev):
            return collect_rows(plan[j]['meta'], plan[j]['slots'], *received, prev, j, n_tab, rows_dev, n_dev)

        served_0 = serve(0, d_out)
        rows_0 = fetch(0, *served_0, d_out)
        x_a, m_a, a_0 = fwd_layers(x_1, w_up, w_down, w_gate, 1, 1, 0, False, served_0[1])
        served_1 = serve(1, m_a)
        x_2 = mix_rows(plan[0]['more'], ids_col, slots_row, *rows_0, (x_a, m_a, a_0), w_proj, 0)
        rows_1 = fetch(1, *served_1, x_2)
        x_b, h_b, a_1 = fwd_layers(x_2, w_up, w_down, w_gate, 2, layers - 2, 1, True, x_2)
        e_1 = mix_rows(plan[1]['more'], ids_col, slots_row, *rows_1, None, w_proj, 1)
        *sums_1, d_a = grad_rows(plan[1]['more'], ids_row, slots_col, d_out, a_1, e_1, w_proj, 1, n_main, n_over)
        recv_1 = give_back(1, *sums_1)
        c_b = bwd_layers(d_out, x_b, h_b, w_up, w_down, d_a, w_gate, layers - 1, 1)
        last = functools.partial(grad_rows, plan[0]['more'], ids_row, slots_col, c_b, a_0, None, w_proj, 0, n_main, n_over)
        over_0, more_0 = last(after=recv_1[:2], kind="over")
        (main_0,) = last(after=(over_0,), kind="main")
        sums_0 = (main_0, over_0, more_0)
        recv_0 = give_back(0, *sums_0)
        x_end = finish(main_0, x_b, h_b, a_1, e_1, w_down, w_proj, layers - 1, 1)
        grads = collect(0, recv_0, collect(1, recv_1, None))
        return x_end, grads

    return jax.shard_map(local_program, mesh=mesh, in_specs=(tok_spec, tok_spec, tab_spec, P(), P(), P(), P(), tab_spec), out_specs=(tok_spec, tab_spec), check_vma=False)
```
